32 devices in a mesh: dp: 4 (over x, core), fsdp: 8 (over z, y).
Axes of the slice: x: 2, y: 2, z: 4, core: 2. Of those that a mesh axis runs over, the one named last changes fastest.
Arguments:
- pixels: bfloat16 [50176, 768], P(('dp', 'fsdp')), may hold values from -6 to 6
- resolution: int32 [256], P(('dp', 'fsdp')), may hold values from 0 to 2, as said below
- kept: int32 [12544], P(('dp', 'fsdp')), may hold values from 0 to 1567, as said below
- step_count: int32 [1], replicated, may hold values from 2 to 20
- encoder_in: float32 [768, 7424], P(('dp', 'fsdp')), may hold values from -0.21875 to 0.21875
- encoder_out: float32 [3072, 768], P(('dp', 'fsdp')), may hold values from -0.109375 to 0.109375
- decoder_in: float32 [512, 4864], P(('dp', 'fsdp')), may hold values from -0.25 to 0.25
- decoder_out: float32 [2048, 512], P(('dp', 'fsdp')), may hold values from -0.125 to 0.125
- norm_gains: float32 [3840], P(('dp', 'fsdp')), may hold values from 0.5 to 1.5
- all_biases: float32 [16640], P(('dp', 'fsdp')), may hold values from -2.4 to 2.4
- moment_encoder_in: float32 [768, 7424], P(('dp', 'fsdp')), may hold values from -4.172325e-07 to 4.172325e-07
- moment_encoder_out: float32 [3072, 768], P(('dp', 'fsdp')), may hold values from -4.172325e-07 to 4.172325e-07
- moment_decoder_in: float32 [512, 4864], P(('dp', 'fsdp')), may hold values from -4.172325e-07 to 4.172325e-07
- moment_decoder_out: float32 [2048, 512], P(('dp', 'fsdp')), may hold values from -4.172325e-07 to 4.172325e-07
- moment_gains: float32 [3840], P(('dp', 'fsdp')), may hold values from -1.66893e-06 to 1.66893e-06
- moment_biases: float32 [16640], P(('dp', 'fsdp')), may hold values from -1.66893e-06 to 1.66893e-06
- square_encoder_in: float32 [768, 7424], P(('dp', 'fsdp')), may hold values from 1.1319536e-14 to 1.8008353e-13
- square_encoder_out: float32 [3072, 768], P(('dp', 'fsdp')), may hold values from 1.1319536e-14 to 1.8008353e-13
- square_decoder_in: float32 [512, 4864], P(('dp', 'fsdp')), may hold values from 1.1319536e-14 to 1.8008353e-13
- square_decoder_out: float32 [2048, 512], P(('dp', 'fsdp')), may hold values from 1.1319536e-14 to 1.8008353e-13
- square_gains: float32 [3840], P(('dp', 'fsdp')), may hold values from 1.8008353e-13 to 2.8813364e-12
- square_biases: float32 [16640], P(('dp', 'fsdp')), may hold values from 1.8008353e-13 to 2.8813364e-12
Outputs:
- loss: float32 [], replicated
- grad_norm: float32 [], replicated
- updated_encoder_in: float32 [768, 7424], P(('dp', 'fsdp'))
- updated_encoder_out: float32 [3072, 768], P(('dp', 'fsdp'))
- updated_decoder_in: float32 [512, 4864], P(('dp', 'fsdp'))
- updated_decoder_out: float32 [2048, 512], P(('dp', 'fsdp'))
- updated_gains: float32 [3840], P(('dp', 'fsdp'))
- updated_biases: float32 [16640], P(('dp', 'fsdp'))
- updated_moment_encoder_in: float32 [768, 7424], P(('dp', 'fsdp'))
- updated_moment_encoder_out: float32 [3072, 768], P(('dp', 'fsdp'))
- updated_moment_decoder_in: float32 [512, 4864], P(('dp', 'fsdp'))
- updated_moment_decoder_out: float32 [2048, 512], P(('dp', 'fsdp'))
- updated_moment_gains: float32 [3840], P(('dp', 'fsdp'))
- updated_moment_biases: float32 [16640], P(('dp', 'fsdp'))
- updated_square_encoder_in: float32 [768, 7424], P(('dp', 'fsdp'))
- updated_square_encoder_out: float32 [3072, 768], P(('dp', 'fsdp'))
- updated_square_decoder_in: float32 [512, 4864], P(('dp', 'fsdp'))
- updated_square_decoder_out: float32 [2048, 512], P(('dp', 'fsdp'))
- updated_square_gains: float32 [3840], P(('dp', 'fsdp'))
- updated_square_biases: float32 [16640], P(('dp', 'fsdp'))
The draws below stay inside these ranges and needn't reach their ends.
Inputs may be any that keep to these rules, and one draw needn't show every extreme that they name: `resolution`: each device's 8 entries, in a random order, are k of class 1, 4 * (2 - k) of class 0 and 3 * k of class 2, for some k from 0 to 2, so that its images fill its 1568 patches exactly. One device has k = 2 and another k = 0. `kept`: each device's 392 entries are distinct indices of its own patches in rising order, exactly a quarter of the patches of every one of its images.
All inputs are finite; a program needn't handle non-finite values.
Results may differ from the reference program's by a relative error of at most 0.0003.
The reference program's roundings to bfloat16 on the way (of `work`) count: a program that leaves them out, or rounds other values in their place, can miss the bound.
Values may be sent and summed in bfloat16 or wider, within the bound.
A program may use at most 256 MiB of HBM per device.

```python
import math
import jax
import jax.numpy as jnp
from jax import lax

D = 768
HEADS = 12
FF = 3072
DD = 512
DHEADS = 16
DFF = 2048
PIX = 768
SIDE_BIG = 28
SIDE_SMALL = 14
UNITS = 2
PATCH_DEV = 1568
KEEP_DEV = 392
SLOTS = 8
PATCHES_ALL = 50176
ENC_COLS = 7424
DEC_COLS = 4864
GAIN_LEN = 3840
BIAS_LEN = 16640
NPARAM = 11620352
N_DP = 4
N_FSDP = 8
DEVICES = 32


def slot_classes(key):
    bigs = jax.random.randint(jax.random.fold_in(key, 11), (DEVICES,), 0, UNITS + 1)
    bigs = bigs.at[0].set(UNITS).at[1].set(0)
    slot_ids = jnp.arange(SLOTS, dtype=jnp.int32)[None, :]
    base = jnp.where(slot_ids < bigs[:, None], 1, jnp.where(slot_ids < bigs[:, None] + 4 * (UNITS - bigs[:, None]), 0, 2))
    scores = jax.random.randint(jax.random.fold_in(key, 12), (DEVICES, SLOTS), 0, 4096) * SLOTS + slot_ids
    order = jnp.argsort(scores, axis=1)
    return jnp.take_along_axis(base, order, axis=1).astype(jnp.int32)


def draw_resolution(key, part):
    return slot_classes(key).reshape(DEVICES * SLOTS)


def kept_one(classes, scores):
    slot_ids = jnp.arange(SLOTS, dtype=jnp.int32)
    lengths = jnp.where(classes == 1, SIDE_BIG * SIDE_BIG, jnp.where(classes == 0, SIDE_SMALL * SIDE_SMALL, 0)).astype(jnp.int32)
    starts = jnp.cumsum(lengths) - lengths
    position = jnp.arange(PATCH_DEV, dtype=jnp.int32)
    inside = (position[:, None] >= starts[None, :]) & (position[:, None] < (starts + lengths)[None, :])
    image = jnp.sum(jnp.where(inside, slot_ids[None, :], 0), axis=1)
    sort_key = image * (1024 * PATCH_DEV) + scores * PATCH_DEV + position
    sorted_index = jnp.argsort(sort_key)
    sorted_image = image[sorted_index]
    rank = position - starts[sorted_image]
    chosen = (rank < (lengths // 4)[sorted_image]).astype(jnp.int32)
    flags = jnp.zeros((PATCH_DEV,), jnp.int32).at[sorted_index].set(chosen)
    order = jnp.argsort((1 - flags) * PATCH_DEV + position)
    return order[:KEEP_DEV].astype(jnp.int32)


def draw_kept(key, part):
    classes = slot_classes(key)
    scores = jax.random.randint(jax.random.fold_in(key, 13), (DEVICES, PATCH_DEV), 0, 1024)
    return jax.vmap(kept_one)(classes, scores).reshape(DEVICES * KEEP_DEV)


def steps_of(own_key, shape, shards, smallest, top_value):
    loudness = 1.0
    for dim, blocks in shards:
        steps = jax.random.uniform(jax.random.fold_in(jax.random.fold_in(own_key, 6), dim), (blocks,), jnp.float32, smallest / len(shards), top_value / len(shards))
        loudness = loudness * jnp.repeat(jnp.exp(steps), shape[dim] // blocks).reshape((-1,) + (1,) * (len(shape) - 1 - dim))
    return loudness


def normal_values(stream_key, shape, scale, limit, cuts=(), held_as=jnp.bfloat16):
    level = steps_of(stream_key, shape, cuts, -0.22, 0.18) if cuts else 1.0
    drawn = jax.random.normal(stream_key, shape, jnp.float32) * scale * level
    return jnp.minimum(jnp.maximum(drawn, -limit), limit).astype(held_as)


def setup_inputs(seed: int = 0) -> dict:
    streams_of = jax.random.split(jax.random.key(seed), 23)
    pixels = normal_values(streams_of[0], (PATCHES_ALL, PIX), 1.0, 6.0, ((0, 32),))
    resolution = draw_resolution(jax.random.fold_in(streams_of[22], 71), 0)
    kept = draw_kept(jax.random.fold_in(streams_of[22], 71), 0)
    step_count = jax.random.randint(streams_of[3], (1,), 2, 21).astype(jnp.int32)
    encoder_in = normal_values(streams_of[4], (D, ENC_COLS), D ** -0.5, 0.21875, ((0, 32),), jnp.float32)
    encoder_out = normal_values(streams_of[5], (FF, D), FF ** -0.5, 0.109375, ((0, 32),), jnp.float32)
    decoder_in = normal_values(streams_of[6], (DD, DEC_COLS), DD ** -0.5, 0.25, ((0, 32),), jnp.float32)
    decoder_out = normal_values(streams_of[7], (DFF, DD), DFF ** -0.5, 0.125, ((0, 32),), jnp.float32)
    norm_gains = jnp.clip(1.0 + 0.1 * jax.random.normal(streams_of[8], (GAIN_LEN,), jnp.float32), 0.5, 1.5)
    all_biases = normal_values(streams_of[9], (BIAS_LEN,), 0.4, 2.4, ((0, 32),), jnp.float32)
    moment_encoder_in = normal_values(streams_of[10], (D, ENC_COLS), (0.055 * (PATCHES_ALL * NPARAM) ** -0.5), 4.172325134277344e-07, ((0, 32),), jnp.float32)
    moment_encoder_out = normal_values(streams_of[11], (FF, D), (0.055 * (PATCHES_ALL * NPARAM) ** -0.5), 4.172325134277344e-07, ((0, 32),), jnp.float32)
    moment_decoder_in = normal_values(streams_of[12], (DD, DEC_COLS), (0.055 * (PATCHES_ALL * NPARAM) ** -0.5), 4.172325134277344e-07, ((0, 32),), jnp.float32)
    moment_decoder_out = normal_values(streams_of[13], (DFF, DD), (0.055 * (PATCHES_ALL * NPARAM) ** -0.5), 4.172325134277344e-07, ((0, 32),), jnp.float32)
    moment_gains = normal_values(streams_of[14], (GAIN_LEN,), (0.22 * (PATCHES_ALL * NPARAM) ** -0.5), 1.6689300537109375e-06, ((0, 32),), jnp.float32)
    moment_biases = normal_values(streams_of[15], (BIAS_LEN,), (0.22 * (PATCHES_ALL * NPARAM) ** -0.5), 1.6689300537109375e-06, ((0, 32),), jnp.float32)
    square_encoder_in = jnp.clip(jnp.exp(math.log(1.8008352784242704e-13) - 2.7668907 * jax.random.uniform(streams_of[16], (D, ENC_COLS), jnp.float32) ** steps_of(streams_of[16], (D, ENC_COLS), ((0, 32),), -0.2, 0.2)), 1.1319535701836709e-14, 1.8008352784242704e-13)
    square_encoder_out = jnp.clip(jnp.exp(math.log(1.8008352784242704e-13) - 2.7668907 * jax.random.uniform(streams_of[17], (FF, D), jnp.float32) ** steps_of(streams_of[17], (FF, D), ((0, 32),), -0.2, 0.2)), 1.1319535701836709e-14, 1.8008352784242704e-13)
    square_decoder_in = jnp.clip(jnp.exp(math.log(1.8008352784242704e-13) - 2.7668907 * jax.random.uniform(streams_of[18], (DD, DEC_COLS), jnp.float32) ** steps_of(streams_of[18], (DD, DEC_COLS), ((0, 32),), -0.2, 0.2)), 1.1319535701836709e-14, 1.8008352784242704e-13)
    square_decoder_out = jnp.clip(jnp.exp(math.log(1.8008352784242704e-13) - 2.7668907 * jax.random.uniform(streams_of[19], (DFF, DD), jnp.float32) ** steps_of(streams_of[19], (DFF, DD), ((0, 32),), -0.2, 0.2)), 1.1319535701836709e-14, 1.8008352784242704e-13)
    square_gains = jnp.clip(jnp.exp(math.log(2.8813364454788326e-12) - 2.7725887 * jax.random.uniform(streams_of[20], (GAIN_LEN,), jnp.float32) ** steps_of(streams_of[20], (GAIN_LEN,), ((0, 32),), -0.2, 0.2)), 1.8008352784242704e-13, 2.8813364454788326e-12)
    square_biases = jnp.clip(jnp.exp(math.log(2.8813364454788326e-12) - 2.7725887 * jax.random.uniform(streams_of[21], (BIAS_LEN,), jnp.float32) ** steps_of(streams_of[21], (BIAS_LEN,), ((0, 32),), -0.2, 0.2)), 1.8008352784242704e-13, 2.8813364454788326e-12)
    return dict(pixels=pixels, resolution=resolution, kept=kept, step_count=step_count, encoder_in=encoder_in, encoder_out=encoder_out, decoder_in=decoder_in, decoder_out=decoder_out, norm_gains=norm_gains, all_biases=all_biases, moment_encoder_in=moment_encoder_in, moment_encoder_out=moment_encoder_out, moment_decoder_in=moment_decoder_in, moment_decoder_out=moment_decoder_out, moment_gains=moment_gains, moment_biases=moment_biases, square_encoder_in=square_encoder_in, square_encoder_out=square_encoder_out, square_decoder_in=square_decoder_in, square_decoder_out=square_decoder_out, square_gains=square_gains, square_biases=square_biases)


@jax.custom_vjp
def low(v):
    return lax.optimization_barrier(v.astype(jnp.bfloat16)).astype(jnp.float32)

@jax.custom_vjp
def low_back(v):
    return v

def low_keep(v):
    return (low(v), None)

def low_pass(kept, grad):
    return (grad,)

def back_keep(v):
    return (v, None)

def back_low(kept, grad):
    return (low(grad),)
low.defvjp(low_keep, low_pass)
low_back.defvjp(back_keep, back_low)
BETA_ONE = 0.9
BETA_TWO = 0.95
EPSILON = 1e-08
RATE = 0.05
DECAY = 0.05

def matmul(left, right):
    return jnp.dot(left, right, precision=lax.Precision.HIGHEST)

def both(value):
    return low(low_back(value))

def pieces(vector, widths):
    result = []
    start = 0
    for width in widths:
        result.append(vector[..., start:start + width])
        start += width
    return result

def layout(resolution, count):
    slot_ids = jnp.arange(resolution.shape[0], dtype=jnp.int32)
    lengths = jnp.where(resolution == 1, SIDE_BIG * SIDE_BIG, jnp.where(resolution == 0, SIDE_SMALL * SIDE_SMALL, 0)).astype(jnp.int32)
    sides = jnp.where(resolution == 1, SIDE_BIG, SIDE_SMALL).astype(jnp.int32)
    starts = jnp.cumsum(lengths) - lengths
    position = jnp.arange(count, dtype=jnp.int32)[:, None]
    inside = (position >= starts[None, :]) & (position < (starts + lengths)[None, :])
    image = lax.optimization_barrier(jnp.sum(jnp.where(inside, slot_ids[None, :], 0), axis=1))
    place = lax.optimization_barrier(jnp.sum(jnp.where(inside, position - starts[None, :], 0), axis=1))
    side = lax.optimization_barrier(jnp.sum(jnp.where(inside, sides[None, :], 0), axis=1))
    return (image, place // side, place % side)

def sine_table(row_pos, col_pos, width):
    quarter = width // 4
    omega = 1.0 / 10000.0 ** (jnp.arange(quarter, dtype=jnp.float32) / quarter)
    across = row_pos.astype(jnp.float32)[:, None] * omega[None, :]
    downward = col_pos.astype(jnp.float32)[:, None] * omega[None, :]
    return jnp.concatenate([jnp.sin(across), jnp.cos(across), jnp.sin(downward), jnp.cos(downward)], axis=1)

def layer_norm(stream, gain, shift):
    centered = stream - lax.optimization_barrier(jnp.mean(stream, axis=1, keepdims=True))
    spread = lax.optimization_barrier(jnp.mean(centered * centered, axis=1, keepdims=True))
    return centered * lax.rsqrt(spread + 1e-06) * gain + shift

def attend(queries, key_rows, values, image, heads):
    count, width = queries.shape
    size = width // heads
    scale = 1.0 / math.sqrt(size)
    same = image[:, None] == image[None, :]

    def split_heads(tensor):
        return tensor.reshape(count, heads, size).transpose(1, 0, 2)

    def one_head(trio):
        query_head, key_head, value_head = trio
        scores = low_back(matmul(query_head, key_head.T) * scale)
        scores = jnp.where(same, scores, -1e+30)
        shifted = jnp.exp(scores - lax.optimization_barrier(jnp.max(scores, axis=1, keepdims=True)))
        weights = low(shifted / lax.optimization_barrier(jnp.sum(shifted, axis=1, keepdims=True)))
        return matmul(weights, value_head)
    mixed = lax.map(jax.checkpoint(one_head), (split_heads(queries), split_heads(key_rows), split_heads(values)))
    return mixed.transpose(1, 0, 2).reshape(count, width)

def block(stream, image, params, heads):
    gain_one, shift_one, w_qkv, bias_query, bias_value, w_out, bias_out, gain_two, shift_two, w_up, bias_up, w_down, bias_down = params
    width = stream.shape[1]
    normed = low(layer_norm(stream, gain_one, shift_one))
    joined = matmul(normed, w_qkv)
    queries = both(joined[:, :width] + bias_query)
    key_rows = both(joined[:, width:2 * width])
    values = both(joined[:, 2 * width:] + bias_value)
    mixed = both(attend(queries, key_rows, values, image, heads))
    stream = stream + low_back(matmul(mixed, w_out) + bias_out)
    normed = low(layer_norm(stream, gain_two, shift_two))
    hidden = low_back(matmul(normed, w_up) + bias_up)
    return stream + low_back(matmul(low(jax.nn.gelu(hidden, approximate=False)), w_down) + bias_down)

def section_a(mats, gain_vec, bias_vec, pixel_rows, kept, resolution):
    w_patch, w_qkv, w_out, w_up, w_lift = pieces(mats[0], (D, 3 * D, D, FF, DD))
    gain_one, gain_two, gain_final = pieces(gain_vec, (D, D, D))
    bias_patch, shift_one, bias_query, bias_value, bias_out, shift_two, bias_up, bias_down, shift_final, bias_lift, mask_token = pieces(bias_vec, (D, D, D, D, D, D, FF, D, D, DD, DD))
    count = pixel_rows.shape[0]
    image, rows, cols = layout(resolution, count)
    stream = low_back(matmul(pixel_rows[kept], w_patch) + bias_patch) + sine_table(rows[kept], cols[kept], D)
    stream = block(stream, image[kept], (gain_one, shift_one, w_qkv, bias_query, bias_value, w_out, bias_out, gain_two, shift_two, w_up, bias_up, mats[1], bias_down), HEADS)
    lifted = low_back(matmul(low(layer_norm(stream, gain_final, shift_final)), w_lift) + bias_lift)
    full = jnp.broadcast_to(mask_token[None, :], (count, DD)).at[kept].set(lifted)
    return full + sine_table(rows, cols, DD)

def section_b(mats, gain_vec, bias_vec, stream, pixel_rows, kept, resolution, denom):
    w_qkv, w_out, w_up, w_head = pieces(mats[0], (3 * DD, DD, DFF, PIX))
    gain_one, gain_two, gain_final = pieces(gain_vec[3 * D:], (DD, DD, DD))
    shift_one, bias_query, bias_value, bias_out, shift_two, bias_up, bias_down, shift_final, bias_head = pieces(bias_vec[8 * D + FF + 2 * DD:], (DD, DD, DD, DD, DD, DFF, DD, DD, PIX))
    count = pixel_rows.shape[0]
    image, rows, cols = layout(resolution, count)
    stream = block(stream, image, (gain_one, shift_one, w_qkv, bias_query, bias_value, w_out, bias_out, gain_two, shift_two, w_up, bias_up, mats[1], bias_down), DHEADS)
    predicted = low_back(matmul(low(layer_norm(stream, gain_final, shift_final)), w_head) + bias_head)
    centered = pixel_rows - lax.optimization_barrier(jnp.mean(pixel_rows, axis=1, keepdims=True))
    target = centered * lax.rsqrt(lax.optimization_barrier(jnp.mean(centered * centered, axis=1, keepdims=True)) + 1e-06)
    error = lax.optimization_barrier(jnp.mean((predicted - target) ** 2, axis=1))
    weight = jnp.ones((count,), jnp.float32).at[kept].set(0.1)
    return jnp.sum(error * weight) / denom

def adamw(weight, grad, first, second, decay, times):
    first_new = BETA_ONE * first + (1.0 - BETA_ONE) * grad
    second_new = BETA_TWO * second + (1.0 - BETA_TWO) * grad * grad
    first_hat = first_new / (1.0 - BETA_ONE ** times)
    second_hat = second_new / (1.0 - BETA_TWO ** times)
    weight_new = weight - RATE * (first_hat / (jnp.sqrt(second_hat) + EPSILON) + decay * weight)
    return (weight_new, first_new, second_new)

def reference(pixels, resolution, kept, step_count, encoder_in, encoder_out, decoder_in, decoder_out, norm_gains, all_biases, moment_encoder_in, moment_encoder_out, moment_decoder_in, moment_decoder_out, moment_gains, moment_biases, square_encoder_in, square_encoder_out, square_decoder_in, square_decoder_out, square_gains, square_biases):
    devices = N_DP * N_FSDP
    denom = (0.75 + 0.1 * 0.25) * PATCHES_ALL
    pixel_blocks = pixels.astype(jnp.float32).reshape(devices, PATCH_DEV, PIX)
    slot_blocks = resolution.reshape(devices, SLOTS)
    kept_blocks = kept.reshape(devices, KEEP_DEV)
    masters = (encoder_in, encoder_out, decoder_in, decoder_out, norm_gains, all_biases)

    def total(params):
        work = [low(weight) for weight in params]

        def one_device(carry, data):
            pixel_rows, slot_row, kept_row = data
            lifted = section_a((work[0], work[1]), work[4], work[5], pixel_rows, kept_row, slot_row)
            return (carry + section_b((work[2], work[3]), work[4], work[5], lifted, pixel_rows, kept_row, slot_row, denom), None)
        return lax.scan(jax.checkpoint(one_device), jnp.zeros((), jnp.float32), (pixel_blocks, slot_blocks, kept_blocks))[0]
    loss, pullback = jax.vjp(total, masters)
    grads = pullback(jnp.ones((), jnp.float32))[0]
    grad_norm = jnp.sqrt(sum((jnp.sum(grad * grad) for grad in grads)))
    factor = jnp.minimum(1.0, 0.5 / math.sqrt(PATCHES_ALL) / (grad_norm + 1e-06))
    times = step_count[0].astype(jnp.float32)
    firsts = (moment_encoder_in, moment_encoder_out, moment_decoder_in, moment_decoder_out, moment_gains, moment_biases)
    seconds = (square_encoder_in, square_encoder_out, square_decoder_in, square_decoder_out, square_gains, square_biases)
    results = [adamw(masters[index], grads[index] * factor, firsts[index], seconds[index], DECAY if index < 4 else 0.0, times) for index in range(6)]
    return (loss, grad_norm, results[0][0], results[1][0], results[2][0], results[3][0], results[4][0], results[5][0], results[0][1], results[1][1], results[2][1], results[3][1], results[4][1], results[5][1], results[0][2], results[1][2], results[2][2], results[3][2], results[4][2], results[5][2])
```

```python
import functools
import math

import jax
import jax.numpy as jnp
from jax import lax
from jax.experimental import pallas as pl
from jax.experimental.pallas import tpu as pltpu
from jax.sharding import PartitionSpec as P

D = 768
HEADS = 12
FF = 3072
DD = 512
DHEADS = 16
DFF = 2048
PIX = 768
SIDE_BIG = 28
SIDE_SMALL = 14


BETA_ONE = 0.9
BETA_TWO = 0.95
EPSILON = 1e-08
RATE = 0.05
DECAY = 0.05


def round_plain(value):
    return lax.optimization_barrier(value.astype(jnp.bfloat16)).astype(jnp.float32)


def value_fwd(value):
    return (round_plain(value), None)


def value_bwd(unused, grad):
    return (grad,)


def identity_plain(value):
    return value


def grad_fwd(value):
    return (value, None)


def grad_bwd(unused, grad):
    return (round_plain(grad),)


def make_rounders():
    value_rule = jax.custom_vjp(round_plain)
    value_rule.defvjp(value_fwd, value_bwd)
    grad_rule = jax.custom_vjp(identity_plain)
    grad_rule.defvjp(grad_fwd, grad_bwd)
    return (value_rule, grad_rule)


def value_round(value):
    return make_rounders()[0](value)


def grad_round(value):
    return make_rounders()[1](value)


def matmul(left, right):
    return jnp.dot(left, right, preferred_element_type=jnp.float32)


def both(value):
    return value_round(grad_round(value))


def pieces(vector, widths):
    result = []
    start = 0
    for width in widths:
        result.append(vector[..., start : start + width])
        start += width
    return result


def layout(resolution, kept, count):
    big, small = SIDE_BIG * SIDE_BIG, SIDE_SMALL * SIDE_SMALL
    ratio = big // small
    units = count // small
    is_big = (resolution == 1).astype(jnp.int32)
    is_small = (resolution == 0).astype(jnp.int32)
    bigs = jnp.sum(is_big)
    lengths = ratio * is_big + is_small
    slots = jnp.arange(resolution.shape[0], dtype=jnp.int32)
    before = slots[:, None] > slots[None, :]

    def earlier(values):
        return jnp.sum(jnp.where(before, values[None, :], 0), axis=1)

    old_start = earlier(lengths)
    new_start = jnp.where(resolution == 1, ratio * earlier(is_big), ratio * bigs + earlier(is_small))
    unit = jnp.arange(units, dtype=jnp.int32)[:, None]
    inside = (unit >= old_start[None, :]) & (unit < (old_start + lengths)[None, :])
    new_of_old = jnp.sum(jnp.where(inside, unit + (new_start - old_start)[None, :], 0), axis=1)
    old_of_new = jnp.sum(jnp.where(unit == new_of_old[None, :], jnp.arange(units, dtype=jnp.int32)[None, :], 0), axis=1)
    kept_unit = kept // small
    matches = kept_unit[:, None] == jnp.arange(units, dtype=jnp.int32)[None, :]
    kept_new = jnp.sum(jnp.where(matches, new_of_old[None, :], 0), axis=1) * small + kept % small

    def places(position):
        whole = position < bigs * big
        place = jnp.where(whole, position % big, position % small)
        side = jnp.where(whole, SIDE_BIG, SIDE_SMALL)
        row = place // side
        part = (position % big) // small
        return (row, place - row * side, jnp.where(whole, 0, part), position // big)

    return places, old_of_new, kept_new


def sine_table(row_pos, col_pos, width):
    quarter = width // 4
    omega = 1.0 / 10000.0 ** (jnp.arange(quarter, dtype=jnp.float32) / quarter)
    across = row_pos.astype(jnp.float32)[:, None] * omega[None, :]
    downward = col_pos.astype(jnp.float32)[:, None] * omega[None, :]
    return jnp.concatenate(
        [jnp.sin(across), jnp.cos(across), jnp.sin(downward), jnp.cos(downward)], axis=1
    )


def layer_norm(stream, gain, shift):
    centered = stream - jnp.mean(stream, axis=1, keepdims=True)
    spread = jnp.mean(centered * centered, axis=1, keepdims=True)
    return centered * lax.rsqrt(spread + 1e-06) * gain + shift


LOG2E = 1.4426950408889634
SEGMENTS = 16
FAR = -1e30
CONTRACT_ROWS = (((0,), (0,)), ((), ()))
CONTRACT_PLAIN = (((1,), (0,)), ((), ()))
CONTRACT_LANES = (((1,), (1,)), ((), ()))


def tile_dot(left, right, dims):
    return lax.dot_general(left, right, dims, preferred_element_type=jnp.float32)


def attend_fwd_kernel(heads, size, q_ref, k_ref, v_ref, away_ref, own_ref, o_ref, lse_ref):
    factor = LOG2E / math.sqrt(size)
    away, own = away_ref[0], own_ref[0]

    def one_head(head, carry):
        rows = pl.ds(pl.multiple_of(head * size, size), size)
        queries = jnp.concatenate([q_ref[0, rows, :], away], axis=0)
        keys = jnp.concatenate([k_ref[0, rows, :], own], axis=0)
        scores = tile_dot(keys, queries, CONTRACT_ROWS)
        top = jnp.max(scores, axis=0, keepdims=True)
        shifted = jnp.exp2((scores - top) * factor)
        total = jnp.sum(shifted, axis=0, keepdims=True)
        weights = (shifted * (1.0 / total)).astype(jnp.bfloat16)
        o_ref[0, rows, :] = tile_dot(v_ref[0, rows, :], weights, CONTRACT_PLAIN).astype(o_ref.dtype)
        lse_ref[0, pl.ds(head, 1), :] = top * factor + jnp.log2(total)
        return carry

    lax.fori_loop(0, heads, one_head, 0)


def attend_bwd_kernel(
    heads, size, q_ref, k_ref, v_ref, do_ref, lse_ref, away_ref, own_ref, dq_ref, dk_ref, dv_ref
):
    scale = 1.0 / math.sqrt(size)
    factor = LOG2E * scale
    away, own = away_ref[0], own_ref[0]

    def one_head(head, carry):
        rows = pl.ds(pl.multiple_of(head * size, size), size)
        q_rows, k_rows, do_rows = q_ref[0, rows, :], k_ref[0, rows, :], do_ref[0, rows, :]
        queries = jnp.concatenate([q_rows, away], axis=0)
        keys = jnp.concatenate([k_rows, own], axis=0)
        scores = tile_dot(keys, queries, CONTRACT_ROWS)
        weights = jnp.exp2(scores * factor - lse_ref[0, pl.ds(head, 1), :])
        spread = tile_dot(v_ref[0, rows, :], do_rows, CONTRACT_ROWS)
        product = weights * spread
        inner = jnp.sum(product, axis=0, keepdims=True)
        dscores = (product - weights * inner).astype(jnp.bfloat16)
        rounded = weights.astype(jnp.bfloat16)
        dv_ref[0, rows, :] = tile_dot(do_rows, rounded, CONTRACT_LANES).astype(dv_ref.dtype)
        dk_ref[0, rows, :] = (tile_dot(q_rows, dscores, CONTRACT_LANES) * scale).astype(dk_ref.dtype)
        dq_ref[0, rows, :] = (tile_dot(k_rows, dscores, CONTRACT_PLAIN) * scale).astype(dq_ref.dtype)
        return carry

    lax.fori_loop(0, heads, one_head, 0)


def attend_specs(groups, width, count, heads):
    size = width // heads
    step = 8 if heads % 8 == 0 else heads
    wide = pl.BlockSpec((1, step * size, count), lambda g, i: (g, i, 0))
    stats = pl.BlockSpec((1, step, count), lambda g, i: (g, i, 0))
    marks = pl.BlockSpec((1, SEGMENTS, count), lambda g, i: (g, 0, 0))
    return size, step, (groups, heads // step), wide, stats, marks


def attend_forward(queries, keys, values, away, own, heads):
    groups, width, count = queries.shape
    size, step, grid, wide, stats, marks = attend_specs(groups, width, count, heads)
    return pl.pallas_call(
        functools.partial(attend_fwd_kernel, step, size),
        grid=grid,
        in_specs=[wide, wide, wide, marks, marks],
        out_specs=[wide, stats],
        out_shape=[
            jax.ShapeDtypeStruct((groups, width, count), jnp.bfloat16),
            jax.ShapeDtypeStruct((groups, heads, count), jnp.float32),
        ],
        compiler_params=pltpu.CompilerParams(vmem_limit_bytes=60 << 20),
        cost_estimate=pl.CostEstimate(
            flops=4 * groups * width * count * count,
            bytes_accessed=8 * groups * width * count,
            transcendentals=groups * heads * count * count,
        ),
        name="attend_forward",
    )(queries, keys, values, away, own)


def attend_backward(queries, keys, values, grads, lse, away, own, heads):
    groups, width, count = queries.shape
    size, step, grid, wide, stats, marks = attend_specs(groups, width, count, heads)
    shape = jax.ShapeDtypeStruct((groups, width, count), jnp.bfloat16)
    return pl.pallas_call(
        functools.partial(attend_bwd_kernel, step, size),
        grid=grid,
        in_specs=[wide, wide, wide, wide, stats, marks, marks],
        out_specs=[wide, wide, wide],
        out_shape=[shape, shape, shape],
        compiler_params=pltpu.CompilerParams(vmem_limit_bytes=60 << 20),
        cost_estimate=pl.CostEstimate(
            flops=10 * groups * width * count * count,
            bytes_accessed=14 * groups * width * count,
            transcendentals=groups * heads * count * count,
        ),
        name="attend_backward",
    )(queries, keys, values, grads, lse, away, own)


def attend_plain(heads, queries, keys, values, away, own):
    return attend_keep(heads, queries, keys, values, away, own)[0]


def attend_keep(heads, queries, keys, values, away, own):
    queries, keys, values = (t.astype(jnp.bfloat16) for t in (queries, keys, values))
    mixed, lse = attend_forward(queries, keys, values, away, own, heads)
    return mixed.astype(jnp.float32), (queries, keys, values, lse, away, own)


def attend_pull(heads, saved, grad):
    queries, keys, values, lse, away, own = saved
    dq, dk, dv = attend_backward(queries, keys, values, grad.astype(jnp.bfloat16), lse, away, own, heads)
    none = jnp.zeros_like(away)
    return tuple(t.astype(jnp.float32) for t in (dq, dk, dv)) + (none, none)


def attend(queries, keys, values, marks, heads):
    rule = jax.custom_vjp(attend_plain, nondiff_argnums=(0,))
    rule.defvjp(attend_keep, attend_pull)
    return rule(heads, queries, keys, values, marks[0], marks[1])


def gelu(value):
    return 0.5 * value * (1.0 + lax.erf(value * math.sqrt(0.5)))


def segment_marks(segment, groups):
    segment = segment.reshape(groups, 1, -1)
    hot = segment == jnp.arange(SEGMENTS, dtype=jnp.int32)[None, :, None]
    return (jnp.where(hot, 0.0, 1.0).astype(jnp.bfloat16), jnp.where(hot, FAR, 0.0).astype(jnp.bfloat16))


def block(stream, marks, params, heads):
    (
        gain_one,
        shift_one,
        w_qkv,
        bias_query,
        bias_value,
        w_out,
        bias_out,
        gain_two,
        shift_two,
        w_up,
        bias_up,
        w_down,
        bias_down,
    ) = params
    width = stream.shape[1]
    groups = marks[0].shape[0]
    normed = value_round(layer_norm(stream, gain_one, shift_one)).reshape(groups, -1, width)
    joined = jnp.einsum("gtd,df->gft", normed, w_qkv, preferred_element_type=jnp.float32)
    queries = both(joined[:, :width] + bias_query[None, :, None])
    key_rows = both(joined[:, width : 2 * width])
    values = both(joined[:, 2 * width :] + bias_value[None, :, None])
    mixed = both(attend(queries, key_rows, values, marks, heads))
    projected = jnp.einsum("gft,fd->gtd", mixed, w_out, preferred_element_type=jnp.float32).reshape(-1, width)
    stream = stream + grad_round(projected + bias_out)
    normed = value_round(layer_norm(stream, gain_two, shift_two))
    hidden = grad_round(matmul(normed, w_up) + bias_up)
    return stream + grad_round(
        matmul(value_round(gelu(hidden)), w_down) + bias_down
    )


def section_a(mats, gain_vec, bias_vec, pixel_rows, kept, order):
    w_patch, w_qkv, w_out, w_up, w_lift = pieces(mats[0], (D, 3 * D, D, FF, DD))
    gain_one, gain_two, gain_final = pieces(gain_vec, (D, D, D))
    (
        bias_patch,
        shift_one,
        bias_query,
        bias_value,
        bias_out,
        shift_two,
        bias_up,
        bias_down,
        shift_final,
        bias_lift,
        mask_token,
    ) = pieces(bias_vec, (D, D, D, D, D, D, FF, D, D, DD, DD))
    count = pixel_rows.shape[0]
    places, unused, kept_new = order
    rows, cols, part, run = places(kept_new)
    stream = grad_round(matmul(pixel_rows[kept], w_patch) + bias_patch) + sine_table(rows, cols, D)
    runs = count // (SIDE_BIG * SIDE_BIG)
    stream = block(
        stream,
        segment_marks(part * runs + run, 1),
        (
            gain_one,
            shift_one,
            w_qkv,
            bias_query,
            bias_value,
            w_out,
            bias_out,
            gain_two,
            shift_two,
            w_up,
            bias_up,
            mats[1],
            bias_down,
        ),
        HEADS,
    )
    lifted = grad_round(
        matmul(value_round(layer_norm(stream, gain_final, shift_final)), w_lift) + bias_lift
    )
    full = jnp.broadcast_to(mask_token[None, :], (count, DD)).at[kept_new].set(lifted)
    rows, cols, part, run = places(jnp.arange(count, dtype=jnp.int32))
    return full + sine_table(rows, cols, DD)


def section_b(mats, gain_vec, bias_vec, stream, pixel_rows, order, denom):
    w_qkv, w_out, w_up, w_head = pieces(mats[0], (3 * DD, DD, DFF, PIX))
    gain_one, gain_two, gain_final = pieces(gain_vec[3 * D :], (DD, DD, DD))
    (
        shift_one,
        bias_query,
        bias_value,
        bias_out,
        shift_two,
        bias_up,
        bias_down,
        shift_final,
        bias_head,
    ) = pieces(bias_vec[8 * D + FF + 2 * DD :], (DD, DD, DD, DD, DD, DFF, DD, DD, PIX))
    count = pixel_rows.shape[0]
    places, old_of_new, kept_new = order
    rows, cols, part, run = places(jnp.arange(count, dtype=jnp.int32))
    stream = block(
        stream,
        segment_marks(part, count // (SIDE_BIG * SIDE_BIG)),
        (
            gain_one,
            shift_one,
            w_qkv,
            bias_query,
            bias_value,
            w_out,
            bias_out,
            gain_two,
            shift_two,
            w_up,
            bias_up,
            mats[1],
            bias_down,
        ),
        DHEADS,
    )
    predicted = grad_round(
        matmul(value_round(layer_norm(stream, gain_final, shift_final)), w_head) + bias_head
    )
    units = pixel_rows.reshape(-1, SIDE_SMALL * SIDE_SMALL, PIX)
    pixel_rows = units[old_of_new].reshape(count, PIX).astype(jnp.float32)
    centered = pixel_rows - jnp.mean(pixel_rows, axis=1, keepdims=True)
    target = centered * lax.rsqrt(jnp.mean(centered * centered, axis=1, keepdims=True) + 1e-06)
    error = jnp.mean((predicted - target) ** 2, axis=1)
    chosen = jnp.any(jnp.arange(count, dtype=jnp.int32)[:, None] == kept_new[None, :], axis=1)
    weight = jnp.where(chosen, 0.1, 1.0)
    return jnp.sum(error * weight) / denom


def adamw(weight, grad, first, second, decay, times):
    first_new = BETA_ONE * first + (1.0 - BETA_ONE) * grad
    second_new = BETA_TWO * second + (1.0 - BETA_TWO) * grad * grad
    first_hat = first_new / (1.0 - BETA_ONE**times)
    second_hat = second_new / (1.0 - BETA_TWO**times)
    weight_new = weight - RATE * (first_hat / (jnp.sqrt(second_hat) + EPSILON) + decay * weight)
    return (weight_new, first_new, second_new)


def widen(arrays):
    return tuple((array.astype(jnp.float32) for array in arrays))


def per_device(
    pixels,
    resolution,
    kept,
    step_count,
    encoder_in,
    encoder_out,
    decoder_in,
    decoder_out,
    norm_gains,
    all_biases,
    moment_encoder_in,
    moment_encoder_out,
    moment_decoder_in,
    moment_decoder_out,
    moment_gains,
    moment_biases,
    square_encoder_in,
    square_encoder_out,
    square_decoder_in,
    square_decoder_out,
    square_gains,
    square_biases,
):
    devices = lax.axis_size("dp") * lax.axis_size("fsdp")
    patches_all = pixels.shape[0] * devices
    denom = (0.75 + 0.1 * 0.25) * patches_all
    order = layout(resolution, kept, pixels.shape[0])
    cotangent = jnp.ones((), jnp.float32)

    def forward_a(mats, gain_vec, bias_vec):
        return section_a(mats, gain_vec, bias_vec, pixels, kept, order)

    def forward_b(mats, gain_vec, bias_vec, stream):
        return section_b(mats, gain_vec, bias_vec, stream, pixels, order, denom)

    encoder_whole = widen(
        (
            lax.all_gather(encoder_in.astype(jnp.bfloat16), ("dp", "fsdp"), axis=0, tiled=True),
            lax.all_gather(encoder_out.astype(jnp.bfloat16), ("dp", "fsdp"), axis=0, tiled=True),
            lax.all_gather(norm_gains.astype(jnp.bfloat16), ("dp", "fsdp"), axis=0, tiled=True),
            lax.all_gather(all_biases.astype(jnp.bfloat16), ("dp", "fsdp"), axis=0, tiled=True),
        )
    )
    encoder_mats = encoder_whole[:2]
    gains_full, biases_full = (encoder_whole[2], encoder_whole[3])
    lifted = forward_a(encoder_mats, gains_full, biases_full)
    loss_local = forward_b(
        widen(
            (
                lax.all_gather(decoder_in.astype(jnp.bfloat16), ("dp", "fsdp"), axis=0, tiled=True),
                lax.all_gather(
                    decoder_out.astype(jnp.bfloat16), ("dp", "fsdp"), axis=0, tiled=True
                ),
            )
        ),
        gains_full,
        biases_full,
        lifted,
    )
    loss_total = lax.psum(loss_local, ("dp", "fsdp"))
    decoder_again = widen(
        (
            lax.all_gather(decoder_in.astype(jnp.bfloat16), ("dp", "fsdp"), axis=0, tiled=True),
            lax.all_gather(decoder_out.astype(jnp.bfloat16), ("dp", "fsdp"), axis=0, tiled=True),
        )
    )
    unused, pull_decoder = jax.vjp(forward_b, decoder_again, gains_full, biases_full, lifted)
    decoder_terms, gain_back, bias_back, stream_back = pull_decoder(cotangent)
    decoder_grads = (
        lax.psum_scatter(decoder_terms[0], ("dp", "fsdp"), scatter_dimension=0, tiled=True),
        lax.psum_scatter(decoder_terms[1], ("dp", "fsdp"), scatter_dimension=0, tiled=True),
    )
    encoder_again = widen(
        (
            lax.all_gather(encoder_in.astype(jnp.bfloat16), ("dp", "fsdp"), axis=0, tiled=True),
            lax.all_gather(encoder_out.astype(jnp.bfloat16), ("dp", "fsdp"), axis=0, tiled=True),
        )
    )
    unused, pull_encoder = jax.vjp(forward_a, encoder_again, gains_full, biases_full)
    encoder_terms, gain_front, bias_front = pull_encoder(stream_back)
    encoder_grads = (
        lax.psum_scatter(encoder_terms[0], ("dp", "fsdp"), scatter_dimension=0, tiled=True),
        lax.psum_scatter(encoder_terms[1], ("dp", "fsdp"), scatter_dimension=0, tiled=True),
        lax.psum_scatter(gain_front + gain_back, ("dp", "fsdp"), scatter_dimension=0, tiled=True),
        lax.psum_scatter(bias_front + bias_back, ("dp", "fsdp"), scatter_dimension=0, tiled=True),
    )
    grads = (
        encoder_grads[0],
        encoder_grads[1],
        decoder_grads[0],
        decoder_grads[1],
        encoder_grads[2],
        encoder_grads[3],
    )
    squares = sum((jnp.sum(grad * grad) for grad in grads))
    total_squares = lax.psum(squares, ("dp", "fsdp"))
    grad_norm = jnp.sqrt(total_squares)
    factor = jnp.minimum(1.0, 0.5 / math.sqrt(patches_all) / (grad_norm + 1e-06))
    times = step_count[0].astype(jnp.float32)
    masters = (encoder_in, encoder_out, decoder_in, decoder_out, norm_gains, all_biases)
    firsts = (
        moment_encoder_in,
        moment_encoder_out,
        moment_decoder_in,
        moment_decoder_out,
        moment_gains,
        moment_biases,
    )
    seconds = (
        square_encoder_in,
        square_encoder_out,
        square_decoder_in,
        square_decoder_out,
        square_gains,
        square_biases,
    )
    results = [
        adamw(
            masters[index],
            grads[index] * factor,
            firsts[index],
            seconds[index],
            DECAY if index < 4 else 0.0,
            times,
        )
        for index in range(6)
    ]
    return (
        loss_total,
        grad_norm,
        results[0][0],
        results[1][0],
        results[2][0],
        results[3][0],
        results[4][0],
        results[5][0],
        results[0][1],
        results[1][1],
        results[2][1],
        results[3][1],
        results[4][1],
        results[5][1],
        results[0][2],
        results[1][2],
        results[2][2],
        results[3][2],
        results[4][2],
        results[5][2],
    )


def solution(mesh):
    in_specs = (
        P(("dp", "fsdp"), None),
        P(("dp", "fsdp")),
        P(("dp", "fsdp")),
        P(),
        P(("dp", "fsdp"), None),
        P(("dp", "fsdp"), None),
        P(("dp", "fsdp"), None),
        P(("dp", "fsdp"), None),
        P(("dp", "fsdp")),
        P(("dp", "fsdp")),
        P(("dp", "fsdp"), None),
        P(("dp", "fsdp"), None),
        P(("dp", "fsdp"), None),
        P(("dp", "fsdp"), None),
        P(("dp", "fsdp")),
        P(("dp", "fsdp")),
        P(("dp", "fsdp"), None),
        P(("dp", "fsdp"), None),
        P(("dp", "fsdp"), None),
        P(("dp", "fsdp"), None),
        P(("dp", "fsdp")),
        P(("dp", "fsdp")),
    )
    out_specs = (
        P(),
        P(),
        P(("dp", "fsdp"), None),
        P(("dp", "fsdp"), None),
        P(("dp", "fsdp"), None),
        P(("dp", "fsdp"), None),
        P(("dp", "fsdp")),
        P(("dp", "fsdp")),
        P(("dp", "fsdp"), None),
        P(("dp", "fsdp"), None),
        P(("dp", "fsdp"), None),
        P(("dp", "fsdp"), None),
        P(("dp", "fsdp")),
        P(("dp", "fsdp")),
        P(("dp", "fsdp"), None),
        P(("dp", "fsdp"), None),
        P(("dp", "fsdp"), None),
        P(("dp", "fsdp"), None),
        P(("dp", "fsdp")),
        P(("dp", "fsdp")),
    )
    return jax.shard_map(
        per_device, mesh=mesh, in_specs=in_specs, out_specs=out_specs, check_vma=False
    )
```

```python
import functools
import math

import jax
import jax.numpy as jnp
from jax import lax
from jax.experimental import pallas as pl
from jax.experimental.pallas import tpu as pltpu
from jax.sharding import PartitionSpec as P

D = 768
HEADS = 12
FF = 3072
DD = 512
DHEADS = 16
DFF = 2048
PIX = 768
SIDE_BIG = 28
SIDE_SMALL = 14


BETA_ONE = 0.9
BETA_TWO = 0.95
EPSILON = 1e-08
RATE = 0.05
DECAY = 0.05


def round_plain(value):
    return lax.optimization_barrier(value.astype(jnp.bfloat16)).astype(jnp.float32)


def value_fwd(value):
    return (round_plain(value), None)


def value_bwd(unused, grad):
    return (grad,)


def identity_plain(value):
    return value


def grad_fwd(value):
    return (value, None)


def grad_bwd(unused, grad):
    return (round_plain(grad),)


def make_rounders():
    value_rule = jax.custom_vjp(round_plain)
    value_rule.defvjp(value_fwd, value_bwd)
    grad_rule = jax.custom_vjp(identity_plain)
    grad_rule.defvjp(grad_fwd, grad_bwd)
    return (value_rule, grad_rule)


def value_round(value):
    return make_rounders()[0](value)


def grad_round(value):
    return make_rounders()[1](value)


def matmul(left, right):
    return jnp.dot(left, right, preferred_element_type=jnp.float32)


def both(value):
    return value_round(grad_round(value))


def pieces(vector, widths):
    result = []
    start = 0
    for width in widths:
        result.append(vector[..., start : start + width])
        start += width
    return result


def layout(resolution, kept, count):
    big, small = SIDE_BIG * SIDE_BIG, SIDE_SMALL * SIDE_SMALL
    ratio = big // small
    units = count // small
    is_big = (resolution == 1).astype(jnp.int32)
    is_small = (resolution == 0).astype(jnp.int32)
    bigs = jnp.sum(is_big)
    lengths = ratio * is_big + is_small
    slots = jnp.arange(resolution.shape[0], dtype=jnp.int32)
    before = slots[:, None] > slots[None, :]

    def earlier(values):
        return jnp.sum(jnp.where(before, values[None, :], 0), axis=1)

    old_start = earlier(lengths)
    new_start = jnp.where(resolution == 1, ratio * earlier(is_big), ratio * bigs + earlier(is_small))
    unit = jnp.arange(units, dtype=jnp.int32)[:, None]
    inside = (unit >= old_start[None, :]) & (unit < (old_start + lengths)[None, :])
    new_of_old = jnp.sum(jnp.where(inside, unit + (new_start - old_start)[None, :], 0), axis=1)
    old_of_new = jnp.sum(jnp.where(unit == new_of_old[None, :], jnp.arange(units, dtype=jnp.int32)[None, :], 0), axis=1)
    kept_unit = kept // small
    matches = kept_unit[:, None] == jnp.arange(units, dtype=jnp.int32)[None, :]
    kept_new = jnp.sum(jnp.where(matches, new_of_old[None, :], 0), axis=1) * small + kept % small

    def places(position):
        whole = position < bigs * big
        place = jnp.where(whole, position % big, position % small)
        side = jnp.where(whole, SIDE_BIG, SIDE_SMALL)
        row = place // side
        part = (position % big) // small
        return (row, place - row * side, jnp.where(whole, 0, part), position // big)

    return places, old_of_new, kept_new


def sine_table(row_pos, col_pos, width):
    quarter = width // 4
    omega = 1.0 / 10000.0 ** (jnp.arange(quarter, dtype=jnp.float32) / quarter)
    across = row_pos.astype(jnp.float32)[:, None] * omega[None, :]
    downward = col_pos.astype(jnp.float32)[:, None] * omega[None, :]
    return jnp.concatenate(
        [jnp.sin(across), jnp.cos(across), jnp.sin(downward), jnp.cos(downward)], axis=1
    )


def layer_norm(stream, gain, shift):
    centered = stream - jnp.mean(stream, axis=1, keepdims=True)
    spread = jnp.mean(centered * centered, axis=1, keepdims=True)
    return centered * lax.rsqrt(spread + 1e-06) * gain + shift


LOG2E = 1.4426950408889634
SEGMENTS = 16
FAR = -1e30
CONTRACT_ROWS = (((0,), (0,)), ((), ()))
CONTRACT_PLAIN = (((1,), (0,)), ((), ()))
CONTRACT_LANES = (((1,), (1,)), ((), ()))


def tile_dot(left, right, dims):
    return lax.dot_general(left, right, dims, preferred_element_type=jnp.float32)


def attend_fwd_kernel(heads, size, q_ref, k_ref, v_ref, away_ref, own_ref, o_ref, lse_ref):
    factor = LOG2E / math.sqrt(size)
    away, own = away_ref[0], own_ref[0]

    def one_head(head, carry):
        rows = pl.ds(pl.multiple_of(head * size, size), size)
        queries = jnp.concatenate([q_ref[0, rows, :], away], axis=0)
        keys = jnp.concatenate([k_ref[0, rows, :], own], axis=0)
        scores = tile_dot(keys, queries, CONTRACT_ROWS)
        top = jnp.max(scores, axis=0, keepdims=True)
        shifted = jnp.exp2((scores - top) * factor)
        total = jnp.sum(shifted, axis=0, keepdims=True)
        weights = (shifted * (1.0 / total)).astype(jnp.bfloat16)
        o_ref[0, rows, :] = tile_dot(v_ref[0, rows, :], weights, CONTRACT_PLAIN).astype(o_ref.dtype)
        lse_ref[0, pl.ds(head, 1), :] = top * factor + jnp.log2(total)
        return carry

    lax.fori_loop(0, heads, one_head, 0)


def attend_bwd_kernel(
    heads, size, q_ref, k_ref, v_ref, do_ref, lse_ref, away_ref, own_ref, dq_ref, dk_ref, dv_ref
):
    scale = 1.0 / math.sqrt(size)
    factor = LOG2E * scale
    away, own = away_ref[0], own_ref[0]

    def one_head(head, carry):
        rows = pl.ds(pl.multiple_of(head * size, size), size)
        q_rows, k_rows, do_rows = q_ref[0, rows, :], k_ref[0, rows, :], do_ref[0, rows, :]
        queries = jnp.concatenate([q_rows, away], axis=0)
        keys = jnp.concatenate([k_rows, own], axis=0)
        scores = tile_dot(keys, queries, CONTRACT_ROWS)
        weights = jnp.exp2(scores * factor - lse_ref[0, pl.ds(head, 1), :])
        spread = tile_dot(v_ref[0, rows, :], do_rows, CONTRACT_ROWS)
        product = weights * spread
        inner = jnp.sum(product, axis=0, keepdims=True)
        dscores = (product - weights * inner).astype(jnp.bfloat16)
        rounded = weights.astype(jnp.bfloat16)
        dv_ref[0, rows, :] = tile_dot(do_rows, rounded, CONTRACT_LANES).astype(dv_ref.dtype)
        dk_ref[0, rows, :] = (tile_dot(q_rows, dscores, CONTRACT_LANES) * scale).astype(dk_ref.dtype)
        dq_ref[0, rows, :] = (tile_dot(k_rows, dscores, CONTRACT_PLAIN) * scale).astype(dq_ref.dtype)
        return carry

    lax.fori_loop(0, heads, one_head, 0)


def attend_specs(groups, width, count, heads):
    size = width // heads
    step = 8 if heads % 8 == 0 else heads
    wide = pl.BlockSpec((1, step * size, count), lambda g, i: (g, i, 0))
    stats = pl.BlockSpec((1, step, count), lambda g, i: (g, i, 0))
    marks = pl.BlockSpec((1, SEGMENTS, count), lambda g, i: (g, 0, 0))
    return size, step, (groups, heads // step), wide, stats, marks


def attend_forward(queries, keys, values, away, own, heads):
    groups, width, count = queries.shape
    size, step, grid, wide, stats, marks = attend_specs(groups, width, count, heads)
    return pl.pallas_call(
        functools.partial(attend_fwd_kernel, step, size),
        grid=grid,
        in_specs=[wide, wide, wide, marks, marks],
        out_specs=[wide, stats],
        out_shape=[
            jax.ShapeDtypeStruct((groups, width, count), jnp.bfloat16),
            jax.ShapeDtypeStruct((groups, heads, count), jnp.float32),
        ],
        compiler_params=pltpu.CompilerParams(vmem_limit_bytes=60 << 20),
        cost_estimate=pl.CostEstimate(
            flops=4 * groups * width * count * count,
            bytes_accessed=8 * groups * width * count,
            transcendentals=groups * heads * count * count,
        ),
        name="attend_forward",
    )(queries, keys, values, away, own)


def attend_backward(queries, keys, values, grads, lse, away, own, heads):
    groups, width, count = queries.shape
    size, step, grid, wide, stats, marks = attend_specs(groups, width, count, heads)
    shape = jax.ShapeDtypeStruct((groups, width, count), jnp.bfloat16)
    return pl.pallas_call(
        functools.partial(attend_bwd_kernel, step, size),
        grid=grid,
        in_specs=[wide, wide, wide, wide, stats, marks, marks],
        out_specs=[wide, wide, wide],
        out_shape=[shape, shape, shape],
        compiler_params=pltpu.CompilerParams(vmem_limit_bytes=60 << 20),
        cost_estimate=pl.CostEstimate(
            flops=10 * groups * width * count * count,
            bytes_accessed=14 * groups * width * count,
            transcendentals=groups * heads * count * count,
        ),
        name="attend_backward",
    )(queries, keys, values, grads, lse, away, own)


def attend_plain(heads, queries, keys, values, away, own):
    return attend_keep(heads, queries, keys, values, away, own)[0]


def attend_keep(heads, queries, keys, values, away, own):
    queries, keys, values = (t.astype(jnp.bfloat16) for t in (queries, keys, values))
    mixed, lse = attend_forward(queries, keys, values, away, own, heads)
    return mixed.astype(jnp.float32), (queries, keys, values, lse, away, own)


def attend_pull(heads, saved, grad):
    queries, keys, values, lse, away, own = saved
    dq, dk, dv = attend_backward(queries, keys, values, grad.astype(jnp.bfloat16), lse, away, own, heads)
    none = jnp.zeros_like(away)
    return tuple(t.astype(jnp.float32) for t in (dq, dk, dv)) + (none, none)


def attend(queries, keys, values, marks, heads):
    rule = jax.custom_vjp(attend_plain, nondiff_argnums=(0,))
    rule.defvjp(attend_keep, attend_pull)
    return rule(heads, queries, keys, values, marks[0], marks[1])


def gelu(value):
    return 0.5 * value * (1.0 + lax.erf(value * math.sqrt(0.5)))


def segment_marks(segment, groups):
    segment = segment.reshape(groups, 1, -1)
    hot = segment == jnp.arange(SEGMENTS, dtype=jnp.int32)[None, :, None]
    return (jnp.where(hot, 0.0, 1.0).astype(jnp.bfloat16), jnp.where(hot, FAR, 0.0).astype(jnp.bfloat16))


def block(stream, marks, params, heads):
    (
        gain_one,
        shift_one,
        w_qkv,
        bias_query,
        bias_value,
        w_out,
        bias_out,
        gain_two,
        shift_two,
        w_up,
        bias_up,
        w_down,
        bias_down,
    ) = params
    width = stream.shape[1]
    groups = marks[0].shape[0]
    normed = value_round(layer_norm(stream, gain_one, shift_one)).reshape(groups, -1, width)
    joined = jnp.einsum("gtd,df->gft", normed, w_qkv, preferred_element_type=jnp.float32)
    queries = both(joined[:, :width] + bias_query[None, :, None])
    key_rows = both(joined[:, width : 2 * width])
    values = both(joined[:, 2 * width :] + bias_value[None, :, None])
    mixed = both(attend(queries, key_rows, values, marks, heads))
    projected = jnp.einsum("gft,fd->gtd", mixed, w_out, preferred_element_type=jnp.float32).reshape(-1, width)
    stream = stream + grad_round(projected + bias_out)
    normed = value_round(layer_norm(stream, gain_two, shift_two))
    hidden = grad_round(matmul(normed, w_up) + bias_up)
    return stream + grad_round(
        matmul(value_round(gelu(hidden)), w_down) + bias_down
    )


def section_a(mats, gain_vec, bias_vec, pixel_rows, kept, order):
    w_patch, w_qkv, w_out, w_up, w_lift = pieces(mats[0], (D, 3 * D, D, FF, DD))
    gain_one, gain_two, gain_final = pieces(gain_vec, (D, D, D))
    (
        bias_patch,
        shift_one,
        bias_query,
        bias_value,
        bias_out,
        shift_two,
        bias_up,
        bias_down,
        shift_final,
        bias_lift,
        mask_token,
    ) = pieces(bias_vec, (D, D, D, D, D, D, FF, D, D, DD, DD))
    count = pixel_rows.shape[0]
    places, unused, kept_new = order
    rows, cols, part, run = places(kept_new)
    stream = grad_round(matmul(pixel_rows[kept], w_patch) + bias_patch) + sine_table(rows, cols, D)
    runs = count // (SIDE_BIG * SIDE_BIG)
    stream = block(
        stream,
        segment_marks(part * runs + run, 1),
        (
            gain_one,
            shift_one,
            w_qkv,
            bias_query,
            bias_value,
            w_out,
            bias_out,
            gain_two,
            shift_two,
            w_up,
            bias_up,
            mats[1],
            bias_down,
        ),
        HEADS,
    )
    lifted = grad_round(
        matmul(value_round(layer_norm(stream, gain_final, shift_final)), w_lift) + bias_lift
    )
    full = jnp.broadcast_to(mask_token[None, :], (count, DD)).at[kept_new].set(lifted)
    rows, cols, part, run = places(jnp.arange(count, dtype=jnp.int32))
    return full + sine_table(rows, cols, DD)


def section_b(mats, gain_vec, bias_vec, stream, pixel_rows, order, denom):
    w_qkv, w_out, w_up, w_head = pieces(mats[0], (3 * DD, DD, DFF, PIX))
    gain_one, gain_two, gain_final = pieces(gain_vec[3 * D :], (DD, DD, DD))
    (
        shift_one,
        bias_query,
        bias_value,
        bias_out,
        shift_two,
        bias_up,
        bias_down,
        shift_final,
        bias_head,
    ) = pieces(bias_vec[8 * D + FF + 2 * DD :], (DD, DD, DD, DD, DD, DFF, DD, DD, PIX))
    count = pixel_rows.shape[0]
    places, old_of_new, kept_new = order
    rows, cols, part, run = places(jnp.arange(count, dtype=jnp.int32))
    stream = block(
        stream,
        segment_marks(part, count // (SIDE_BIG * SIDE_BIG)),
        (
            gain_one,
            shift_one,
            w_qkv,
            bias_query,
            bias_value,
            w_out,
            bias_out,
            gain_two,
            shift_two,
            w_up,
            bias_up,
            mats[1],
            bias_down,
        ),
        DHEADS,
    )
    predicted = grad_round(
        matmul(value_round(layer_norm(stream, gain_final, shift_final)), w_head) + bias_head
    )
    units = pixel_rows.reshape(-1, SIDE_SMALL * SIDE_SMALL, PIX)
    pixel_rows = units[old_of_new].reshape(count, PIX).astype(jnp.float32)
    centered = pixel_rows - jnp.mean(pixel_rows, axis=1, keepdims=True)
    target = centered * lax.rsqrt(jnp.mean(centered * centered, axis=1, keepdims=True) + 1e-06)
    error = jnp.mean((predicted - target) ** 2, axis=1)
    chosen = jnp.any(jnp.arange(count, dtype=jnp.int32)[:, None] == kept_new[None, :], axis=1)
    weight = jnp.where(chosen, 0.1, 1.0)
    return jnp.sum(error * weight) / denom


def adamw(weight, grad, first, second, decay, times):
    first_new = BETA_ONE * first + (1.0 - BETA_ONE) * grad
    second_new = BETA_TWO * second + (1.0 - BETA_TWO) * grad * grad
    first_hat = first_new / (1.0 - BETA_ONE**times)
    second_hat = second_new / (1.0 - BETA_TWO**times)
    weight_new = weight - RATE * (first_hat / (jnp.sqrt(second_hat) + EPSILON) + decay * weight)
    return (weight_new, first_new, second_new)


LANES = 128
AXES = ("dp", "fsdp")
GRID_DIMS = (2, 2, 4, 2)
MESH_IDS = pl.DeviceIdType.MESH


def place_of():
    dp, fsdp = lax.axis_index("dp"), lax.axis_index("fsdp")
    x, core = dp // 2, dp % 2
    z, y = fsdp // 2, fsdp % 2
    flip_x = ((1 - x) * 2 + core, fsdp)
    flip_y = (dp, z * 2 + 1 - y)

    def choose(zero, one):
        return tuple(a * (1 - core) + b * core for a, b in zip(zero, one))

    partners = [(x * 2 + 1 - core, fsdp), choose(flip_x, flip_y), choose(flip_y, flip_x)]
    partners += [(dp, lax.rem(z + step, 4) * 2 + y) for step in (1, 2, 3)]
    return x, core, z, y, partners


def greet(partners):
    barrier = pltpu.get_barrier_semaphore()
    for partner in partners:
        pl.semaphore_signal(barrier, inc=1, device_id=partner, device_id_type=MESH_IDS)
    pl.semaphore_wait(barrier, len(partners))


def column_cuts(columns, parts):
    tiles = columns // LANES
    cuts = [LANES * (tiles * part // parts) for part in range(parts + 1)]
    return [(low, high - low) for low, high in zip(cuts[:-1], cuts[1:])]


def xy_of(core, first, second):
    return first * (1 - core) + second * core, second * (1 - core) + first * core


def scatter_kernel(chunks, slots, arrays, *refs):
    sources, loss_ref = refs[:arrays], refs[arrays]
    outs, total_ref = refs[arrays + 1 : 2 * arrays + 1], refs[2 * arrays + 1]
    scratch = refs[2 * arrays + 2 :]
    count = len(chunks)
    arrive = [scratch[4 * j : 4 * j + 4] for j in range(count)]
    kept = scratch[4 * count : -7]
    own = [kept[slot].at[:, :, pl.ds(0, width)] for slot, width in slots]
    pair, quad, send_sem, recv_sem, own_sem, last_send, last_recv = scratch[-7:]
    x, core, z, y, partners = place_of()
    first, second = xy_of(core, x, y)

    def remote(source, target, j, phase, partner):
        return pltpu.make_async_remote_copy(
            source, target, send_sem.at[j, phase], recv_sem.at[j, phase], device_id=partner, device_id_type=MESH_IDS
        )

    def view(j, side, b1, b2):
        array, low, width = chunks[j]
        at_x, at_y = xy_of(side, b1, b2)
        return sources[array].at[at_x, side, :, at_y, :, pl.ds(low, width)]

    def start_swap(j):
        for b1 in range(2):
            for b2 in range(2):
                place = pl.ds((b1 * 2 + b2) * 4, 4)
                remote(view(j, 1 - core, b1, b2), arrive[j][0].at[place], j, 0, partners[0]).start()

    def start_own(j):
        for b1 in range(2):
            for b2 in range(2):
                place = pl.ds((b1 * 2 + b2) * 4, 4)
                pltpu.make_async_copy(view(j, core, b1, b2), own[j].at[place], own_sem.at[j]).start()

    def whole(j, phase):
        buffer = arrive[j][phase]
        return pltpu.make_async_copy(buffer, buffer, recv_sem.at[j, phase])

    def add_into(target, other, offset, blocks):
        def step(n, carry):
            target[n] = target[n] + other[offset + n]
            return carry

        lax.fori_loop(0, blocks, step, 0)

    sends = []

    def stage_one(j):
        pltpu.make_async_copy(own[j], own[j], own_sem.at[j]).wait()
        whole(j, 0).wait()
        add_into(arrive[j][0], own[j], 0, 16)
        remote(arrive[j][0].at[pl.ds((1 - first) * 8, 8)], arrive[j][1], j, 1, partners[1]).start()

    def stage_two(j):
        whole(j, 1).wait()
        add_into(arrive[j][1], arrive[j][0], first * 8, 8)
        remote(arrive[j][1].at[pl.ds((1 - second) * 4, 4)], arrive[j][2], j, 2, partners[2]).start()

    def stage_three(j):
        whole(j, 2).wait()
        add_into(arrive[j][2], arrive[j][1], second * 4, 4)
        for step in range(3):
            there = lax.rem(z + step + 1, 4)
            remote(arrive[j][2].at[there], arrive[j][3].at[step], j, 3 + step, partners[3 + step]).start()

    def stage_four(j):
        array, low, width = chunks[j]
        for step in range(3):
            slot = arrive[j][3].at[step]
            pltpu.make_async_copy(slot, slot, recv_sem.at[j, 3 + step]).wait()
        result = (arrive[j][2][z] + arrive[j][3][0]) + (arrive[j][3][1] + arrive[j][3][2])
        outs[array][:, low : low + width] = result
        square = result * result
        rows = square.shape[0]
        tile = functools.reduce(
            jnp.add,
            [square[r : r + 8, c : c + LANES] for r in range(0, rows, 8) for c in range(0, width, LANES)],
        )
        pair[0, 0] = pair[0, 0] + tile

    greet(partners)
    pair[0, 0] = jnp.zeros((8, LANES), jnp.float32)
    pair[0, 1] = loss_ref[...]
    ahead = 2
    for j in range(min(ahead, count)):
        start_swap(j)
        start_own(j)
    for t in range(count + 3):
        if t < count:
            if t + ahead < count:
                start_swap(t + ahead)
            stage_one(t)
            if t + ahead < count:
                start_own(t + ahead)
        if 0 <= t - 1 < count:
            stage_two(t - 1)
        if 0 <= t - 2 < count:
            stage_three(t - 2)
        if 0 <= t - 3 < count:
            stage_four(t - 3)

    def share(source, target, n, partner):
        return pltpu.make_async_remote_copy(
            source, target, last_send.at[n], last_recv.at[n], device_id=partner, device_id_type=MESH_IDS
        )

    tail = []
    for n in range(3):
        copy = share(pair.at[n], pair.at[4 + n], n, partners[n])
        copy.start()
        copy.wait_recv()
        tail.append(copy)
        target = pair.at[n + 1] if n < 2 else quad.at[z]
        target[...] = pair[n] + pair[4 + n]
    for step in range(3):
        copy = share(quad.at[z], quad.at[z], 3 + step, partners[3 + step])
        copy.start()
        tail.append(copy)
    for copy in tail[3:]:
        copy.wait_recv()
    total_ref[...] = (quad[0] + quad[1]) + (quad[2] + quad[3])
    for copy in tail:
        copy.wait_send()
    for j in range(count):
        pltpu.make_async_copy(arrive[j][0], arrive[j][0], send_sem.at[j, 0]).wait()
        pltpu.make_async_copy(arrive[j][1], arrive[j][1], send_sem.at[j, 1]).wait()
        pltpu.make_async_copy(arrive[j][2], arrive[j][2], send_sem.at[j, 2]).wait()
        for step in range(3):
            slot = arrive[j][3].at[step]
            pltpu.make_async_copy(slot, slot, send_sem.at[j, 3 + step]).wait()


def scatter_sums(arrays, parts, loss, collective_id):
    sources, chunks, slots, scratch_a, scratch_b = [], [], [], [], []
    for index, (array, cuts) in enumerate(zip(arrays, parts)):
        devices, rows, columns = array.shape
        sources.append(array.reshape(GRID_DIMS + (rows, columns)))
        cut = column_cuts(columns, cuts)
        widest = max(width for low, width in cut)
        base = len(scratch_b)
        scratch_b += [pltpu.VMEM((16, rows, widest), jnp.float32)] * min(2, cuts)
        for number, (low, width) in enumerate(cut):
            chunks.append((index, low, width))
            slots.append((base + number % 2, width))
            scratch_a += [pltpu.VMEM((n, rows, width), jnp.float32) for n in (16, 8, 4, 3)]
    count = len(chunks)
    sent = sum(array.size for array in arrays) * 4
    vmem = pl.BlockSpec(memory_space=pltpu.VMEM)
    return pl.pallas_call(
        functools.partial(scatter_kernel, tuple(chunks), tuple(slots), len(arrays)),
        in_specs=[pl.BlockSpec(memory_space=pl.ANY)] * len(arrays) + [vmem],
        out_specs=[vmem] * (len(arrays) + 1),
        out_shape=[jax.ShapeDtypeStruct(a.shape[1:], jnp.float32) for a in arrays]
        + [jax.ShapeDtypeStruct((2, 8, LANES), jnp.float32)],
        scratch_shapes=scratch_a + scratch_b
        + [
            pltpu.VMEM((7, 2, 8, LANES), jnp.float32),
            pltpu.VMEM((4, 2, 8, LANES), jnp.float32),
            pltpu.SemaphoreType.DMA((count, 6)),
            pltpu.SemaphoreType.DMA((count, 6)),
            pltpu.SemaphoreType.DMA((count,)),
            pltpu.SemaphoreType.DMA((6,)),
            pltpu.SemaphoreType.DMA((6,)),
        ],
        compiler_params=pltpu.CompilerParams(
            collective_id=collective_id, has_side_effects=True, vmem_limit_bytes=63 << 20
        ),
        cost_estimate=pl.CostEstimate(flops=sent // 2, bytes_accessed=3 * sent, transcendentals=0),
        name="scatter_sums",
    )(*sources, loss)


def gather_kernel(chunks, arrays, *refs):
    shards, wholes = refs[:arrays], refs[arrays : 2 * arrays]
    send_sem, recv_sem, own_sem = refs[2 * arrays :]
    x, core, z, y, partners = place_of()
    first, second = xy_of(core, x, y)

    def remote(source, target, j, phase, partner):
        return pltpu.make_async_remote_copy(
            source, target, send_sem.at[j, phase], recv_sem.at[j, phase], device_id=partner, device_id_type=MESH_IDS
        )

    def line(j, b1, b2):
        array, low, width = chunks[j]
        at_x, at_y = xy_of(core, b1, b2)
        return wholes[array].at[at_x, core, :, at_y, :, pl.ds(low, width)]

    def mine(j):
        array, low, width = chunks[j]
        return shards[array].at[:, pl.ds(low, width)], wholes[array].at[x, core, z, y, :, pl.ds(low, width)]

    def along_z(j):
        source, target = mine(j)
        copies = [remote(source, target, j, step, partners[3 + step]) for step in range(3)]
        return copies

    def along_second(j):
        return [remote(line(j, first, second), line(j, first, second), j, 3, partners[2])]

    def along_first(j):
        return [remote(line(j, first, b2), line(j, first, b2), j, 4 + b2, partners[1]) for b2 in range(2)]

    def across(j):
        return [
            remote(line(j, b1, b2), line(j, b1, b2), j, 6 + b1 * 2 + b2, partners[0])
            for b1 in range(2)
            for b2 in range(2)
        ]

    greet(partners)
    count = len(chunks)
    stages = (along_z, along_second, along_first, across)
    flights = [[None] * count for stage in stages]
    for j in range(count):
        source, target = mine(j)
        pltpu.make_async_copy(source, target, own_sem.at[j]).start()
    for t in range(count + len(stages) - 1):
        for s, stage in enumerate(stages):
            j = t - s
            if 0 <= j < count:
                if s == 1:
                    source, target = mine(j)
                    pltpu.make_async_copy(source, target, own_sem.at[j]).wait()
                if s > 0:
                    for copy in flights[s - 1][j]:
                        copy.wait_recv()
                flights[s][j] = stage(j)
                for copy in flights[s][j]:
                    copy.start()
    for j in range(count):
        for copy in flights[-1][j]:
            copy.wait_recv()
    for j in range(count):
        for flight in flights:
            for copy in flight[j]:
                copy.wait_send()


def gather_whole(shards, parts, collective_id):
    chunks = []
    for index, (shard, cuts) in enumerate(zip(shards, parts)):
        chunks += [(index, low, width) for low, width in column_cuts(shard.shape[1], cuts)]
    count = len(chunks)
    wholes = pl.pallas_call(
        functools.partial(gather_kernel, tuple(chunks), len(shards)),
        in_specs=[pl.BlockSpec(memory_space=pltpu.VMEM)] * len(shards),
        out_specs=[pl.BlockSpec(memory_space=pl.ANY)] * len(shards),
        out_shape=[jax.ShapeDtypeStruct(GRID_DIMS + s.shape, s.dtype) for s in shards],
        scratch_shapes=[
            pltpu.SemaphoreType.DMA((count, 10)),
            pltpu.SemaphoreType.DMA((count, 10)),
            pltpu.SemaphoreType.DMA((count,)),
        ],
        compiler_params=pltpu.CompilerParams(
            collective_id=collective_id, has_side_effects=True, vmem_limit_bytes=16 << 20
        ),
        name="gather_whole",
    )(*shards)
    return [w.reshape((math.prod(GRID_DIMS),) + s.shape) for w, s in zip(wholes, shards)]


def widen(arrays):
    return tuple((array.astype(jnp.float32) for array in arrays))


def vector_tile(vectors):
    joined = jnp.concatenate(vectors, axis=-1)
    lead, length = joined.shape[:-1], joined.shape[-1]
    columns = LANES * (-(-length // (8 * LANES)))
    joined = jnp.pad(joined, [(0, 0)] * len(lead) + [(0, 8 * columns - length)])
    return joined.reshape(lead + (8, columns))


def cut_tile(tile, lengths):
    lead = tile.shape[:-2]
    flat = tile.reshape(lead + (-1,))
    return pieces(flat, lengths)


def kernels_fit():
    return (lax.axis_size("dp"), lax.axis_size("fsdp")) == (4, 8)


def gather_weights(matrices, vectors):
    matrices = [m.astype(jnp.bfloat16) for m in matrices]
    vectors = [v.astype(jnp.bfloat16) for v in vectors]
    if not kernels_fit():
        whole = [lax.all_gather(a, AXES, axis=0, tiled=True) for a in matrices + vectors]
        return whole[: len(matrices)], whole[len(matrices) :]
    tile = vector_tile(vectors)
    whole = gather_whole([tile] + matrices, (1,) + GATHER_CUTS, 1)
    cut = cut_tile(whole[0], [v.shape[0] for v in vectors])
    full = [w.reshape((-1, w.shape[-1])) for w in whole[1:]]
    return full, [c.reshape(-1) for c in cut]


def scatter_grads(matrices, vectors, loss):
    if not kernels_fit():
        sums = [lax.psum_scatter(g, AXES, scatter_dimension=0, tiled=True) for g in matrices + vectors]
        squares = sum(jnp.sum(g * g) for g in sums)
        return sums, lax.psum(squares, AXES), lax.psum(loss, AXES)
    devices = math.prod(GRID_DIMS)
    blocks = [m.reshape((devices, -1, m.shape[-1])) for m in matrices]
    tile = vector_tile([v.reshape(devices, -1) for v in vectors])
    corner = lax.broadcasted_iota(jnp.int32, (8, LANES), 0) + lax.broadcasted_iota(jnp.int32, (8, LANES), 1) == 0
    outs = scatter_sums(blocks + [tile], SCATTER_CUTS + (1,), jnp.where(corner, loss, 0.0), 2)
    cut = cut_tile(outs[len(matrices)], [v.shape[0] // devices for v in vectors])
    totals = outs[-1]
    return list(outs[: len(matrices)]) + list(cut), jnp.sum(totals[0]), jnp.sum(totals[1])


GATHER_CUTS = (4, 2, 2, 1)
SCATTER_CUTS = (8, 3, 4, 2)


def per_device(
    pixels,
    resolution,
    kept,
    step_count,
    *state,
):
    masters, firsts, seconds = state[:6], state[6:12], state[12:]
    devices = lax.axis_size("dp") * lax.axis_size("fsdp")
    patches_all = pixels.shape[0] * devices
    denom = (0.75 + 0.1 * 0.25) * patches_all
    order = layout(resolution, kept, pixels.shape[0])

    def forward_a(mats, gain_vec, bias_vec):
        return section_a(mats, gain_vec, bias_vec, pixels, kept, order)

    def forward_b(mats, gain_vec, bias_vec, stream):
        return section_b(mats, gain_vec, bias_vec, stream, pixels, order, denom)

    matrices, vectors = gather_weights(masters[:4], masters[4:])
    matrices, vectors = widen(matrices), widen(vectors)
    lifted, pull_encoder = jax.vjp(forward_a, matrices[:2], *vectors)
    loss_local, pull_decoder = jax.vjp(forward_b, matrices[2:], *vectors, lifted)
    decoder_terms, gain_back, bias_back, stream_back = pull_decoder(jnp.ones((), jnp.float32))
    encoder_terms, gain_front, bias_front = pull_encoder(stream_back)
    grads, total_squares, loss_total = scatter_grads(
        list(encoder_terms) + list(decoder_terms), [gain_front + gain_back, bias_front + bias_back], loss_local
    )
    grad_norm = jnp.sqrt(total_squares)
    factor = jnp.minimum(1.0, 0.5 / math.sqrt(patches_all) / (grad_norm + 1e-06))
    times = step_count[0].astype(jnp.float32)
    results = [
        adamw(
            masters[index],
            grads[index] * factor,
            firsts[index],
            seconds[index],
            DECAY if index < 4 else 0.0,
            times,
        )
        for index in range(6)
    ]
    return (loss_total, grad_norm) + tuple(result[part] for part in range(3) for result in results)


def solution(mesh):
    in_specs = (
        P(("dp", "fsdp"), None),
        P(("dp", "fsdp")),
        P(("dp", "fsdp")),
        P(),
        P(("dp", "fsdp"), None),
        P(("dp", "fsdp"), None),
        P(("dp", "fsdp"), None),
        P(("dp", "fsdp"), None),
        P(("dp", "fsdp")),
        P(("dp", "fsdp")),
        P(("dp", "fsdp"), None),
        P(("dp", "fsdp"), None),
        P(("dp", "fsdp"), None),
        P(("dp", "fsdp"), None),
        P(("dp", "fsdp")),
        P(("dp", "fsdp")),
        P(("dp", "fsdp"), None),
        P(("dp", "fsdp"), None),
        P(("dp", "fsdp"), None),
        P(("dp", "fsdp"), None),
        P(("dp", "fsdp")),
        P(("dp", "fsdp")),
    )
    out_specs = (
        P(),
        P(),
        P(("dp", "fsdp"), None),
        P(("dp", "fsdp"), None),
        P(("dp", "fsdp"), None),
        P(("dp", "fsdp"), None),
        P(("dp", "fsdp")),
        P(("dp", "fsdp")),
        P(("dp", "fsdp"), None),
        P(("dp", "fsdp"), None),
        P(("dp", "fsdp"), None),
        P(("dp", "fsdp"), None),
        P(("dp", "fsdp")),
        P(("dp", "fsdp")),
        P(("dp", "fsdp"), None),
        P(("dp", "fsdp"), None),
        P(("dp", "fsdp"), None),
        P(("dp", "fsdp"), None),
        P(("dp", "fsdp")),
        P(("dp", "fsdp")),
    )
    return jax.shard_map(
        per_device, mesh=mesh, in_specs=in_specs, out_specs=out_specs, check_vma=False
    )
```

```python
import functools
import math

import jax
import jax.numpy as jnp
from jax import lax
from jax.experimental import pallas as pl
from jax.experimental.pallas import tpu as pltpu
from jax.sharding import PartitionSpec as P

D = 768
HEADS = 12
FF = 3072
DD = 512
DHEADS = 16
DFF = 2048
PIX = 768
SIDE_BIG = 28
SIDE_SMALL = 14


BETA_ONE = 0.9
BETA_TWO = 0.95
EPSILON = 1e-08
RATE = 0.05
DECAY = 0.05


def round_plain(value):
    return lax.optimization_barrier(value.astype(jnp.bfloat16)).astype(jnp.float32)


def value_fwd(value):
    return (round_plain(value), None)


def value_bwd(unused, grad):
    return (grad,)


def identity_plain(value):
    return value


def grad_fwd(value):
    return (value, None)


def grad_bwd(unused, grad):
    return (round_plain(grad),)


def make_rounders():
    value_rule = jax.custom_vjp(round_plain)
    value_rule.defvjp(value_fwd, value_bwd)
    grad_rule = jax.custom_vjp(identity_plain)
    grad_rule.defvjp(grad_fwd, grad_bwd)
    return (value_rule, grad_rule)


def value_round(value):
    return make_rounders()[0](value)


def grad_round(value):
    return make_rounders()[1](value)


def matmul(left, right):
    return jnp.dot(left, right, preferred_element_type=jnp.float32)


def both(value):
    return value_round(grad_round(value))


def pieces(vector, widths):
    result = []
    start = 0
    for width in widths:
        result.append(vector[..., start : start + width])
        start += width
    return result


def layout(resolution, kept, count):
    big, small = SIDE_BIG * SIDE_BIG, SIDE_SMALL * SIDE_SMALL
    ratio = big // small
    units = count // small
    is_big = (resolution == 1).astype(jnp.int32)
    is_small = (resolution == 0).astype(jnp.int32)
    bigs = jnp.sum(is_big)
    lengths = ratio * is_big + is_small
    slots = jnp.arange(resolution.shape[0], dtype=jnp.int32)
    before = slots[:, None] > slots[None, :]

    def earlier(values):
        return jnp.sum(jnp.where(before, values[None, :], 0), axis=1)

    old_start = earlier(lengths)
    new_start = jnp.where(resolution == 1, ratio * earlier(is_big), ratio * bigs + earlier(is_small))
    unit = jnp.arange(units, dtype=jnp.int32)[:, None]
    inside = (unit >= old_start[None, :]) & (unit < (old_start + lengths)[None, :])
    new_of_old = jnp.sum(jnp.where(inside, unit + (new_start - old_start)[None, :], 0), axis=1)
    old_of_new = jnp.sum(jnp.where(unit == new_of_old[None, :], jnp.arange(units, dtype=jnp.int32)[None, :], 0), axis=1)
    kept_unit = kept // small
    matches = kept_unit[:, None] == jnp.arange(units, dtype=jnp.int32)[None, :]
    kept_new = jnp.sum(jnp.where(matches, new_of_old[None, :], 0), axis=1) * small + kept % small

    def places(position):
        whole = position < bigs * big
        place = jnp.where(whole, position % big, position % small)
        side = jnp.where(whole, SIDE_BIG, SIDE_SMALL)
        row = place // side
        part = (position % big) // small
        return (row, place - row * side, jnp.where(whole, 0, part), position // big)

    return places, old_of_new, kept_new


def sine_table(row_pos, col_pos, width):
    quarter = width // 4
    reach = 8 * (-(-SIDE_BIG // 8))
    omega = 1.0 / 10000.0 ** (jnp.arange(quarter, dtype=jnp.float32) / quarter)
    angles = jnp.arange(reach, dtype=jnp.float32)[:, None] * omega[None, :]
    half = jnp.concatenate([jnp.sin(angles), jnp.cos(angles)], axis=1)
    none = jnp.zeros_like(half)
    table = jnp.concatenate(
        [jnp.concatenate([half, none], axis=1), jnp.concatenate([none, half], axis=1)], axis=0
    )
    spot = jnp.arange(2 * reach, dtype=jnp.int32)[None, :]
    hot = (spot == row_pos[:, None]) | (spot == col_pos[:, None] + reach)
    return jnp.dot(hot.astype(jnp.float32), table, precision=lax.Precision.HIGHEST)


def layer_norm(stream, gain, shift):
    centered = stream - jnp.mean(stream, axis=1, keepdims=True)
    spread = jnp.mean(centered * centered, axis=1, keepdims=True)
    return centered * lax.rsqrt(spread + 1e-06) * gain + shift


LOG2E = 1.4426950408889634
SEGMENTS = 16
FAR = -1e30
CONTRACT_ROWS = (((0,), (0,)), ((), ()))
CONTRACT_PLAIN = (((1,), (0,)), ((), ()))
CONTRACT_LANES = (((1,), (1,)), ((), ()))


def tile_dot(left, right, dims):
    return lax.dot_general(left, right, dims, preferred_element_type=jnp.float32)


LANES = 128
AXES = ("dp", "fsdp")
GRID_DIMS = (2, 2, 4, 2)
DEVICE_BLOCKS = 32
MESH_IDS = pl.DeviceIdType.MESH
WHOLE_VMEM = pl.BlockSpec(memory_space=pltpu.VMEM)
LEFT_ALONE = pl.BlockSpec(memory_space=pl.ANY)


def place_of():
    dp, fsdp = lax.axis_index("dp"), lax.axis_index("fsdp")
    x, core = dp // 2, dp % 2
    z, y = fsdp // 2, fsdp % 2
    flip_x = ((1 - x) * 2 + core, fsdp)
    flip_y = (dp, z * 2 + 1 - y)

    def choose(zero, one):
        return tuple(a * (1 - core) + b * core for a, b in zip(zero, one))

    partners = [(x * 2 + 1 - core, fsdp), choose(flip_x, flip_y), choose(flip_y, flip_x)]
    partners += [(dp, lax.rem(z + step, 4) * 2 + y) for step in (1, 2, 3)]
    return x, core, z, y, partners


def greet(partners):
    barrier = pltpu.get_barrier_semaphore()
    for partner in partners:
        pl.semaphore_signal(barrier, inc=1, device_id=partner, device_id_type=MESH_IDS)
    pl.semaphore_wait(barrier, len(partners))


def column_cuts(columns, parts):
    tiles = columns // LANES
    cuts = [LANES * (tiles * part // parts) for part in range(parts + 1)]
    return [(low, high - low) for low, high in zip(cuts[:-1], cuts[1:])]


def xy_of(core, first, second):
    return first * (1 - core) + second * core, second * (1 - core) + first * core


class Terms:
    def __init__(self, rows, columns, cuts, array=None, left=None, right=None, dims=None):
        self.rows, self.columns, self.cuts = rows, columns, cuts
        self.array, self.left, self.right, self.dims = array, left, right, dims

    def inputs(self):
        if self.array is None:
            return [(self.left, WHOLE_VMEM), (self.right, WHOLE_VMEM)]
        return [(self.array.reshape(GRID_DIMS + (self.rows, self.columns)), LEFT_ALONE)]


class Scatter:
    def __init__(self, terms, loss=None):
        self.terms, self.loss = terms, loss
        pairs = [pair for term in terms for pair in term.inputs()]
        if loss is not None:
            pairs.append((loss, WHOLE_VMEM))
        self.arrays = [array for array, spec in pairs]
        self.in_specs = [spec for array, spec in pairs]
        self.out_shape = [jax.ShapeDtypeStruct((t.rows, t.columns), jnp.float32) for t in terms]
        if loss is not None:
            self.out_shape.append(jax.ShapeDtypeStruct((2, 8, LANES), jnp.float32))
        self.out_specs = [WHOLE_VMEM] * len(self.out_shape)
        self.chunks, self.slots, landing, kept = [], [], [], []
        kinds, last = {}, {}
        for term in terms:
            kind = (term.rows, term.array is None)
            widest = max(width for low, width in column_cuts(term.columns, term.cuts))
            kinds[kind] = (max(widest, kinds.get(kind, (0, 0))[0]), term.cuts + kinds.get(kind, (0, 0))[1])
        bases = {}
        for kind, (widest, number) in kinds.items():
            bases[kind] = (len(kept), min(2, number))
            dims = GRID_DIMS if kind[1] else (16,)
            kept += [pltpu.VMEM(dims + (kind[0], widest), jnp.float32)] * min(2, number)
        seen = {}
        for index, term in enumerate(terms):
            kind = (term.rows, term.array is None)
            for low, width in column_cuts(term.columns, term.cuts):
                base, number = bases[kind]
                slot = base + seen.get(kind, 0) % number
                seen[kind] = seen.get(kind, 0) + 1
                self.chunks.append((index, low, width, last.get(slot)))
                last[slot] = len(self.chunks) - 1
                self.slots.append((slot, width))
                landing += [pltpu.VMEM((n, term.rows, width), jnp.float32) for n in (16, 8, 4, 3)]
        count = len(self.chunks)
        self.kept = len(kept)
        self.scratch = landing + kept
        if loss is not None:
            self.scratch += [pltpu.VMEM((7, 2, 8, LANES), jnp.float32), pltpu.VMEM((4, 2, 8, LANES), jnp.float32)]
            self.scratch += [pltpu.SemaphoreType.DMA((6,)), pltpu.SemaphoreType.DMA((6,))]
        self.scratch += [
            pltpu.SemaphoreType.DMA((count, 6)),
            pltpu.SemaphoreType.DMA((count, 6)),
            pltpu.SemaphoreType.DMA((count,)),
        ]

    def steps(self, ins, outs, scratch):
        chunks, terms, count = self.chunks, self.terms, len(self.chunks)
        sources, at = [], 0
        for term in terms:
            number = 2 if term.array is None else 1
            sources.append(ins[at : at + number])
            at += number
        arrive = [scratch[4 * j : 4 * j + 4] for j in range(count)]
        kept = scratch[4 * count : 4 * count + self.kept]
        send_sem, recv_sem, own_sem = scratch[-3:]
        x, core, z, y, partners = place_of()
        first, second = xy_of(core, x, y)

        def remote(source, target, j, phase, partner):
            return pltpu.make_async_remote_copy(
                source, target, send_sem.at[j, phase], recv_sem.at[j, phase], device_id=partner, device_id_type=MESH_IDS
            )

        def slot_of(j):
            slot, width = self.slots[j]
            lead = 1 if terms[chunks[j][0]].array is not None else 4
            return kept[slot].at[(slice(None),) * lead + (slice(None), pl.ds(0, width))]

        def view(j, side, b1, b2):
            index, low, width, before = chunks[j]
            at_x, at_y = xy_of(side, b1, b2)
            if terms[index].array is None:
                return slot_of(j).at[at_x, side, :, at_y]
            return sources[index][0].at[at_x, side, :, at_y, :, pl.ds(low, width)]

        def sent(j, phase):
            buffer = arrive[j][min(phase, 3)]
            buffer = buffer.at[phase - 3] if phase >= 3 else buffer
            pltpu.make_async_copy(buffer, buffer, send_sem.at[j, phase]).wait()

        def came(j, phase):
            buffer = arrive[j][min(phase, 3)]
            buffer = buffer.at[phase - 3] if phase >= 3 else buffer
            pltpu.make_async_copy(buffer, buffer, recv_sem.at[j, phase]).wait()

        quarters = [(b1, b2, pl.ds((b1 * 2 + b2) * 4, 4)) for b1 in range(2) for b2 in range(2)]

        def begin(j):
            index, low, width, before = chunks[j]
            term = terms[index]
            if term.array is None:
                if before is not None:
                    sent(before, 0)
                left, right = sources[index]
                piece = right[pl.ds(low, width), :] if term.dims == CONTRACT_LANES else right[:, pl.ds(low, width)]
                product = tile_dot(left[...], piece, term.dims)
                slot_of(j)[...] = product.reshape(GRID_DIMS + (term.rows, width))
            for b1, b2, place in quarters:
                remote(view(j, 1 - core, b1, b2), arrive[j][0].at[place], j, 0, partners[0]).start()
                if term.array is not None:
                    pltpu.make_async_copy(view(j, core, b1, b2), slot_of(j).at[place], own_sem.at[j]).start()

        def add_into(target, other, offset, blocks):
            def step(n, carry):
                target[n] = target[n] + other[offset + n]
                return carry

            lax.fori_loop(0, blocks, step, 0)

        def stage_one(j):
            slot = slot_of(j)
            product = terms[chunks[j][0]].array is None
            if not product:
                pltpu.make_async_copy(slot, slot, own_sem.at[j]).wait()
            came(j, 0)
            if product:
                for b1, b2, place in quarters:
                    at_x, at_y = xy_of(core, b1, b2)
                    for at_z in range(4):
                        n = (b1 * 2 + b2) * 4 + at_z
                        arrive[j][0][n] = arrive[j][0][n] + slot[at_x, core, at_z, at_y]
            else:
                add_into(arrive[j][0], slot, 0, 16)
            remote(arrive[j][0].at[pl.ds((1 - first) * 8, 8)], arrive[j][1], j, 1, partners[1]).start()

        def stage_two(j):
            came(j, 1)
            add_into(arrive[j][1], arrive[j][0], first * 8, 8)
            remote(arrive[j][1].at[pl.ds((1 - second) * 4, 4)], arrive[j][2], j, 2, partners[2]).start()

        def stage_three(j):
            came(j, 2)
            add_into(arrive[j][2], arrive[j][1], second * 4, 4)
            for step in range(3):
                there = lax.rem(z + step + 1, 4)
                remote(arrive[j][2].at[there], arrive[j][3].at[step], j, 3 + step, partners[3 + step]).start()

        def stage_four(j):
            index, low, width, before = chunks[j]
            for step in range(3):
                came(j, 3 + step)
            far = arrive[j][3]
            outs[index][:, low : low + width] = (arrive[j][2][z] + far[0]) + (far[1] + far[2])

        def run(t):
            if t == 0:
                greet(partners)
                begin(0)
            if t + 1 < count:
                begin(t + 1)
            for back, stage in enumerate((stage_one, stage_two, stage_three, stage_four)):
                if 0 <= t - back < count:
                    stage(t - back)

        def finish():
            again = {before for index, low, width, before in chunks if before is not None and terms[index].array is None}
            for j in range(count):
                for phase in range(6):
                    if phase > 0 or j not in again:
                        sent(j, phase)

        def totals():
            pair, quad, last_send, last_recv = scratch[-7:-3]
            loss_ref, total_ref, square_ins = ins[at], outs[-1], ins[at + 1 :]

            def share(source, target, n, partner):
                return pltpu.make_async_remote_copy(
                    source, target, last_send.at[n], last_recv.at[n], device_id=partner, device_id_type=MESH_IDS
                )

            tile = jnp.zeros((8, LANES), jnp.float32)
            for ref in list(outs[: len(terms)]) + list(square_ins):
                square = ref[...] * ref[...]
                rows, columns = square.shape
                tile = functools.reduce(
                    jnp.add,
                    [square[r : r + 8, c : c + LANES] for r in range(0, rows, 8) for c in range(0, columns, LANES)],
                    tile,
                )
            pair[0, 0] = tile
            pair[0, 1] = loss_ref[...]
            tail = []
            for n in range(3):
                copy = share(pair.at[n], pair.at[4 + n], n, partners[n])
                copy.start()
                copy.wait_recv()
                tail.append(copy)
                target = pair.at[n + 1] if n < 2 else quad.at[z]
                target[...] = pair[n] + pair[4 + n]
            for step in range(3):
                copy = share(quad.at[z], quad.at[z], 3 + step, partners[3 + step])
                copy.start()
                tail.append(copy)
            for copy in tail[3:]:
                copy.wait_recv()
            total_ref[...] = (quad[0] + quad[1]) + (quad[2] + quad[3])
            for copy in tail:
                copy.wait_send()

        parts = [functools.partial(run, t) for t in range(count + 3)]
        return parts + ([totals] if self.loss is not None else []) + [finish]


class Gather:
    def __init__(self, shards, cut_pieces):
        self.arrays, self.in_specs = list(shards), [WHOLE_VMEM] * len(shards)
        self.chunks, self.out_shape = [], []
        for shard, low, width, cuts in cut_pieces:
            for start, wide in column_cuts(width, cuts):
                self.chunks.append((shard, low + start, len(self.out_shape), start, wide))
            self.out_shape.append(
                jax.ShapeDtypeStruct(GRID_DIMS + (shards[shard].shape[0], width), shards[shard].dtype)
            )
        self.out_specs = [LEFT_ALONE] * len(self.out_shape)
        count = len(self.chunks)
        self.scratch = [
            pltpu.SemaphoreType.DMA((count, 10)),
            pltpu.SemaphoreType.DMA((count, 10)),
            pltpu.SemaphoreType.DMA((count,)),
        ]

    def steps(self, ins, outs, scratch):
        chunks, count = self.chunks, len(self.chunks)
        send_sem, recv_sem, own_sem = scratch
        x, core, z, y, partners = place_of()
        first, second = xy_of(core, x, y)

        def remote(source, target, j, phase, partner):
            return pltpu.make_async_remote_copy(
                source, target, send_sem.at[j, phase], recv_sem.at[j, phase], device_id=partner, device_id_type=MESH_IDS
            )

        def line(j, b1, b2):
            shard, source, out, low, width = chunks[j]
            at_x, at_y = xy_of(core, b1, b2)
            return outs[out].at[at_x, core, :, at_y, :, pl.ds(low, width)]

        def mine(j):
            shard, source, out, low, width = chunks[j]
            return ins[shard].at[:, pl.ds(source, width)], outs[out].at[x, core, z, y, :, pl.ds(low, width)]

        def own(j):
            source, target = mine(j)
            return pltpu.make_async_copy(source, target, own_sem.at[j])

        def along_z(j):
            source, target = mine(j)
            return [remote(source, target, j, step, partners[3 + step]) for step in range(3)]

        def along_second(j):
            return [remote(line(j, first, second), line(j, first, second), j, 3, partners[2])]

        def along_first(j):
            return [remote(line(j, first, b2), line(j, first, b2), j, 4 + b2, partners[1]) for b2 in range(2)]

        def across(j):
            return [
                remote(line(j, b1, b2), line(j, b1, b2), j, 6 + b1 * 2 + b2, partners[0])
                for b1 in range(2)
                for b2 in range(2)
            ]

        stages = (along_z, along_second, along_first, across)

        def run(t):
            if t == 0:
                greet(partners)
                for j in range(count):
                    own(j).start()
            for s, stage in enumerate(stages):
                j = t - s
                if 0 <= j < count:
                    if s == 1:
                        own(j).wait()
                    if s > 0:
                        for copy in stages[s - 1](j):
                            copy.wait_recv()
                    for copy in stage(j):
                        copy.start()

        def finish():
            for j in range(count):
                for copy in across(j):
                    copy.wait_recv()
            for j in range(count):
                for stage in stages:
                    for copy in stage(j):
                        copy.wait_send()

        return [functools.partial(run, t) for t in range(count + len(stages) - 1)] + [finish]


def run_alone(plan, collective_id, name, more=()):
    def kernel(*refs):
        inputs = len(plan.arrays) + len(more)
        outputs = len(plan.out_shape)
        for step in plan.steps(refs[:inputs], refs[inputs : inputs + outputs], refs[inputs + outputs :]):
            step()

    sent = sum(array.size * array.dtype.itemsize for array in plan.arrays)
    return pl.pallas_call(
        kernel,
        in_specs=plan.in_specs + [WHOLE_VMEM] * len(more),
        out_specs=plan.out_specs,
        out_shape=plan.out_shape,
        scratch_shapes=plan.scratch,
        compiler_params=pltpu.CompilerParams(
            collective_id=collective_id, has_side_effects=True, vmem_limit_bytes=63 << 20
        ),
        cost_estimate=pl.CostEstimate(flops=sent, bytes_accessed=2 * sent, transcendentals=0),
        name=name,
    )(*plan.arrays, *more)


def hosted_refs(refs, inputs, outputs, plan):
    extra_in = len(plan.arrays) if plan else 0
    extra_out = len(plan.out_shape) if plan else 0
    cuts = [inputs, extra_in, outputs, extra_out]
    result, at = [], 0
    for cut in cuts:
        result.append(refs[at : at + cut])
        at += cut
    own_in, plan_in, own_out, plan_out = result
    steps = plan.steps(plan_in, plan_out, refs[at:]) if plan else []
    return own_in, own_out, steps


def host_steps(steps, heads, head, work):
    blocks = pl.num_programs(1)
    now = (pl.program_id(0) * blocks + pl.program_id(1)) * heads + head
    places = {}
    total = 2 * 16
    for number, step in enumerate(steps[:-1]):
        places.setdefault(number * total // (len(steps) - 1), []).append(step)
    for place, group in places.items():

        @pl.when(now == place)
        def start(group=group):
            for step in group:
                step()

    work()
    if steps:
        pl.when(now == total - 1)(steps[-1])


def attend_fwd_kernel(heads, size, plan, *refs):
    (q_ref, k_ref, v_ref, away_ref, own_ref), (o_ref, lse_ref), steps = hosted_refs(refs, 5, 2, plan)
    factor = LOG2E / math.sqrt(size)

    def one_head(head, carry):
        def work():
            rows = pl.ds(pl.multiple_of(head * size, size), size)
            queries = jnp.concatenate([q_ref[0, rows, :], away_ref[0]], axis=0)
            keys = jnp.concatenate([k_ref[0, rows, :], own_ref[0]], axis=0)
            scores = tile_dot(keys, queries, CONTRACT_ROWS)
            top = jnp.max(scores, axis=0, keepdims=True)
            shifted = jnp.exp2((scores - top) * factor)
            total = jnp.sum(shifted, axis=0, keepdims=True)
            weights = (shifted * (1.0 / total)).astype(jnp.bfloat16)
            o_ref[0, rows, :] = tile_dot(v_ref[0, rows, :], weights, CONTRACT_PLAIN).astype(o_ref.dtype)
            lse_ref[0, pl.ds(head, 1), :] = top * factor + jnp.log2(total)

        host_steps(steps, heads, head, work)
        return carry

    lax.fori_loop(0, heads, one_head, 0)


def attend_bwd_kernel(heads, size, plan, *refs):
    ins, (dq_ref, dk_ref, dv_ref), steps = hosted_refs(refs, 7, 3, plan)
    q_ref, k_ref, v_ref, do_ref, lse_ref, away_ref, own_ref = ins
    scale = 1.0 / math.sqrt(size)
    factor = LOG2E * scale

    def one_head(head, carry):
        def work():
            rows = pl.ds(pl.multiple_of(head * size, size), size)
            q_rows, k_rows, do_rows = q_ref[0, rows, :], k_ref[0, rows, :], do_ref[0, rows, :]
            queries = jnp.concatenate([q_rows, away_ref[0]], axis=0)
            keys = jnp.concatenate([k_rows, own_ref[0]], axis=0)
            scores = tile_dot(keys, queries, CONTRACT_ROWS)
            weights = jnp.exp2(scores * factor - lse_ref[0, pl.ds(head, 1), :])
            spread = tile_dot(v_ref[0, rows, :], do_rows, CONTRACT_ROWS)
            product = weights * spread
            inner = jnp.sum(product, axis=0, keepdims=True)
            dscores = (product - weights * inner).astype(jnp.bfloat16)
            rounded = weights.astype(jnp.bfloat16)
            dv_ref[0, rows, :] = tile_dot(do_rows, rounded, CONTRACT_LANES).astype(dv_ref.dtype)
            dk_ref[0, rows, :] = (tile_dot(q_rows, dscores, CONTRACT_LANES) * scale).astype(dk_ref.dtype)
            dq_ref[0, rows, :] = (tile_dot(k_rows, dscores, CONTRACT_PLAIN) * scale).astype(dq_ref.dtype)

        host_steps(steps, heads, head, work)
        return carry

    lax.fori_loop(0, heads, one_head, 0)


def attend_call(kernel, name, wides, lse, marks, heads, outputs, plan, collective_id):
    groups, width, count = wides[0].shape
    size = width // heads
    step = 8 if heads % 8 == 0 else heads
    wide = pl.BlockSpec((1, step * size, count), lambda g, i: (g, i, 0))
    stats = pl.BlockSpec((1, step, count), lambda g, i: (g, i, 0))
    mark = pl.BlockSpec((1, SEGMENTS, count), lambda g, i: (g, 0, 0))
    shape = jax.ShapeDtypeStruct((groups, width, count), jnp.bfloat16)
    ins, in_specs = list(wides), [wide] * len(wides)
    out_specs, out_shape = [wide] * outputs, [shape] * outputs
    if lse is None:
        out_specs.append(stats)
        out_shape.append(jax.ShapeDtypeStruct((groups, heads, count), jnp.float32))
    else:
        ins.append(lse)
        in_specs.append(stats)
    ins += list(marks)
    in_specs += [mark, mark]
    extra = {}
    if plan is not None:
        ins += plan.arrays
        in_specs += plan.in_specs
        out_specs += plan.out_specs
        out_shape += plan.out_shape
        extra = dict(collective_id=collective_id, has_side_effects=True)
    products = 2 if lse is None else 5
    return pl.pallas_call(
        functools.partial(kernel, step, size, plan),
        grid=(groups, heads // step),
        in_specs=in_specs,
        out_specs=out_specs,
        out_shape=out_shape,
        scratch_shapes=plan.scratch if plan is not None else [],
        compiler_params=pltpu.CompilerParams(vmem_limit_bytes=62 << 20, **extra),
        cost_estimate=pl.CostEstimate(
            flops=2 * products * groups * width * count * count,
            bytes_accessed=8 * groups * width * count,
            transcendentals=groups * heads * count * count,
        ),
        name=name,
    )(*ins)


def attend_forward(queries, keys, values, marks, heads, plan=None, collective_id=None):
    outs = attend_call(
        attend_fwd_kernel, "attend_forward", (queries, keys, values), None, marks, heads, 1, plan, collective_id
    )
    return outs[0], outs[1], outs[2:]


def attend_backward(queries, keys, values, grads, lse, marks, heads, plan=None, collective_id=None):
    outs = attend_call(
        attend_bwd_kernel, "attend_backward", (queries, keys, values, grads), lse, marks, heads, 3, plan, collective_id
    )
    return tuple(outs[:3]), outs[3:]


def gelu(value):
    return 0.5 * value * (1.0 + lax.erf(value * math.sqrt(0.5)))


def segment_marks(segment, groups):
    segment = segment.reshape(groups, 1, -1)
    hot = segment == jnp.arange(SEGMENTS, dtype=jnp.int32)[None, :, None]
    return (jnp.where(hot, 0.0, 1.0).astype(jnp.bfloat16), jnp.where(hot, FAR, 0.0).astype(jnp.bfloat16))


def tap_plain(value, spare):
    return value


def tap_fwd(value, spare):
    return (value, None)


def tap_bwd(unused, grad):
    return (grad, grad.astype(jnp.bfloat16))


def tap(value, spare):
    rule = jax.custom_vjp(tap_plain)
    rule.defvjp(tap_fwd, tap_bwd)
    return rule(value, spare)


ENCODER_GAINS = (D, D, D)
ENCODER_BIASES = (D, D, D, D, D, D, FF, D, D, DD, DD)
DECODER_GAINS = (DD, DD, DD)
DECODER_BIASES = (DD, DD, DD, DD, DD, DFF, DD, DD, PIX)
ENCODER_IN = (D, 3 * D, D, FF, DD)
DECODER_IN = (3 * DD, DD, DFF, PIX)


def heads_in(stream, gain, shift, weight, bias_query, bias_value, groups):
    width = stream.shape[1]
    normed = value_round(layer_norm(stream, gain, shift))
    joined = jnp.einsum(
        "gtd,df->gft", normed.reshape(groups, -1, width), weight, preferred_element_type=jnp.float32
    )
    queries = both(joined[:, :width] + bias_query[None, :, None])
    key_rows = both(joined[:, width : 2 * width])
    values = both(joined[:, 2 * width :] + bias_value[None, :, None])
    return (queries, key_rows, values), normed


def encoder_open(gains, biases, spare, pixel_rows, positions, w_patch, w_qkv):
    gain_one = gains[0]
    bias_patch, shift_one, bias_query, bias_value = biases[:4]
    stream = grad_round(tap(matmul(pixel_rows, w_patch), spare) + bias_patch) + positions
    trio, normed = heads_in(stream, gain_one, shift_one, w_qkv, bias_query, bias_value, 1)
    return (trio, stream), normed


def encoder_close(mixed, stream, gains, biases, spares, weights):
    unused, gain_two, gain_final = gains
    bias_out, shift_two, bias_up, bias_down, shift_final, bias_lift = biases[4:10]
    w_out, w_up, w_down, w_lift = weights
    projected = jnp.einsum("gft,fd->gtd", mixed, w_out, preferred_element_type=jnp.float32)
    stream = stream + grad_round(tap(projected[0], spares[0]) + bias_out)
    normed = value_round(layer_norm(stream, gain_two, shift_two))
    hidden = grad_round(tap(matmul(normed, w_up), spares[1]) + bias_up)
    active = value_round(gelu(hidden))
    stream = stream + grad_round(tap(matmul(active, w_down), spares[2]) + bias_down)
    last = value_round(layer_norm(stream, gain_final, shift_final))
    lifted = grad_round(tap(matmul(last, w_lift), spares[3]) + bias_lift)
    return lifted, (normed, active, last)


def decoder_open(lifted, mask_token, gains, biases, kept_new, positions, groups, w_qkv):
    full = jnp.broadcast_to(mask_token[None, :], positions.shape).at[kept_new].set(lifted, unique_indices=True)
    stream = full + positions
    trio, normed = heads_in(stream, gains[0], biases[0], w_qkv, biases[1], biases[2], groups)
    return trio, stream


def decoder_close(mixed, stream, gains, biases, weights, target, weight, denom):
    unused, gain_two, gain_final = gains
    bias_out, shift_two, bias_up, bias_down, shift_final, bias_head = biases[3:]
    w_out, w_up, w_down, w_head = weights
    projected = jnp.einsum("gft,fd->gtd", mixed, w_out, preferred_element_type=jnp.float32)
    stream = stream + grad_round(projected.reshape(stream.shape) + bias_out)
    normed = value_round(layer_norm(stream, gain_two, shift_two))
    hidden = grad_round(matmul(normed, w_up) + bias_up)
    stream = stream + grad_round(matmul(value_round(gelu(hidden)), w_down) + bias_down)
    last = value_round(layer_norm(stream, gain_final, shift_final))
    predicted = grad_round(matmul(last, w_head) + bias_head)
    error = jnp.mean((predicted - target) ** 2, axis=1)
    return jnp.sum(error * weight) / denom


def adamw(weight, grad, first, second, decay, times):
    first_new = BETA_ONE * first + (1.0 - BETA_ONE) * grad
    second_new = BETA_TWO * second + (1.0 - BETA_TWO) * grad * grad
    first_hat = first_new / (1.0 - BETA_ONE**times)
    second_hat = second_new / (1.0 - BETA_TWO**times)
    weight_new = weight - RATE * (first_hat / (jnp.sqrt(second_hat) + EPSILON) + decay * weight)
    return (weight_new, first_new, second_new)


LANES = 128
AXES = ("dp", "fsdp")
GRID_DIMS = (2, 2, 4, 2)
MESH_IDS = pl.DeviceIdType.MESH


def place_of():
    dp, fsdp = lax.axis_index("dp"), lax.axis_index("fsdp")
    x, core = dp // 2, dp % 2
    z, y = fsdp // 2, fsdp % 2
    flip_x = ((1 - x) * 2 + core, fsdp)
    flip_y = (dp, z * 2 + 1 - y)

    def choose(zero, one):
        return tuple(a * (1 - core) + b * core for a, b in zip(zero, one))

    partners = [(x * 2 + 1 - core, fsdp), choose(flip_x, flip_y), choose(flip_y, flip_x)]
    partners += [(dp, lax.rem(z + step, 4) * 2 + y) for step in (1, 2, 3)]
    return x, core, z, y, partners


def greet(partners):
    barrier = pltpu.get_barrier_semaphore()
    for partner in partners:
        pl.semaphore_signal(barrier, inc=1, device_id=partner, device_id_type=MESH_IDS)
    pl.semaphore_wait(barrier, len(partners))


def column_cuts(columns, parts):
    tiles = columns // LANES
    cuts = [LANES * (tiles * part // parts) for part in range(parts + 1)]
    return [(low, high - low) for low, high in zip(cuts[:-1], cuts[1:])]


def xy_of(core, first, second):
    return first * (1 - core) + second * core, second * (1 - core) + first * core


def scatter_kernel(chunks, slots, arrays, *refs):
    sources, loss_ref = refs[:arrays], refs[arrays]
    outs, total_ref = refs[arrays + 1 : 2 * arrays + 1], refs[2 * arrays + 1]
    scratch = refs[2 * arrays + 2 :]
    count = len(chunks)
    arrive = [scratch[4 * j : 4 * j + 4] for j in range(count)]
    kept = scratch[4 * count : -7]
    own = [kept[slot].at[:, :, pl.ds(0, width)] for slot, width in slots]
    pair, quad, send_sem, recv_sem, own_sem, last_send, last_recv = scratch[-7:]
    x, core, z, y, partners = place_of()
    first, second = xy_of(core, x, y)

    def remote(source, target, j, phase, partner):
        return pltpu.make_async_remote_copy(
            source, target, send_sem.at[j, phase], recv_sem.at[j, phase], device_id=partner, device_id_type=MESH_IDS
        )

    def view(j, side, b1, b2):
        array, low, width = chunks[j]
        at_x, at_y = xy_of(side, b1, b2)
        return sources[array].at[at_x, side, :, at_y, :, pl.ds(low, width)]

    def start_swap(j):
        for b1 in range(2):
            for b2 in range(2):
                place = pl.ds((b1 * 2 + b2) * 4, 4)
                remote(view(j, 1 - core, b1, b2), arrive[j][0].at[place], j, 0, partners[0]).start()

    def start_own(j):
        for b1 in range(2):
            for b2 in range(2):
                place = pl.ds((b1 * 2 + b2) * 4, 4)
                pltpu.make_async_copy(view(j, core, b1, b2), own[j].at[place], own_sem.at[j]).start()

    def whole(j, phase):
        buffer = arrive[j][phase]
        return pltpu.make_async_copy(buffer, buffer, recv_sem.at[j, phase])

    def add_into(target, other, offset, blocks):
        def step(n, carry):
            target[n] = target[n] + other[offset + n]
            return carry

        lax.fori_loop(0, blocks, step, 0)

    sends = []

    def stage_one(j):
        pltpu.make_async_copy(own[j], own[j], own_sem.at[j]).wait()
        whole(j, 0).wait()
        add_into(arrive[j][0], own[j], 0, 16)
        remote(arrive[j][0].at[pl.ds((1 - first) * 8, 8)], arrive[j][1], j, 1, partners[1]).start()

    def stage_two(j):
        whole(j, 1).wait()
        add_into(arrive[j][1], arrive[j][0], first * 8, 8)
        remote(arrive[j][1].at[pl.ds((1 - second) * 4, 4)], arrive[j][2], j, 2, partners[2]).start()

    def stage_three(j):
        whole(j, 2).wait()
        add_into(arrive[j][2], arrive[j][1], second * 4, 4)
        for step in range(3):
            there = lax.rem(z + step + 1, 4)
            remote(arrive[j][2].at[there], arrive[j][3].at[step], j, 3 + step, partners[3 + step]).start()

    def stage_four(j):
        array, low, width = chunks[j]
        for step in range(3):
            slot = arrive[j][3].at[step]
            pltpu.make_async_copy(slot, slot, recv_sem.at[j, 3 + step]).wait()
        result = (arrive[j][2][z] + arrive[j][3][0]) + (arrive[j][3][1] + arrive[j][3][2])
        outs[array][:, low : low + width] = result
        square = result * result
        rows = square.shape[0]
        tile = functools.reduce(
            jnp.add,
            [square[r : r + 8, c : c + LANES] for r in range(0, rows, 8) for c in range(0, width, LANES)],
        )
        pair[0, 0] = pair[0, 0] + tile

    greet(partners)
    pair[0, 0] = jnp.zeros((8, LANES), jnp.float32)
    pair[0, 1] = loss_ref[...]
    ahead = 2
    for j in range(min(ahead, count)):
        start_swap(j)
        start_own(j)
    for t in range(count + 3):
        if t < count:
            if t + ahead < count:
                start_swap(t + ahead)
            stage_one(t)
            if t + ahead < count:
                start_own(t + ahead)
        if 0 <= t - 1 < count:
            stage_two(t - 1)
        if 0 <= t - 2 < count:
            stage_three(t - 2)
        if 0 <= t - 3 < count:
            stage_four(t - 3)

    def share(source, target, n, partner):
        return pltpu.make_async_remote_copy(
            source, target, last_send.at[n], last_recv.at[n], device_id=partner, device_id_type=MESH_IDS
        )

    tail = []
    for n in range(3):
        copy = share(pair.at[n], pair.at[4 + n], n, partners[n])
        copy.start()
        copy.wait_recv()
        tail.append(copy)
        target = pair.at[n + 1] if n < 2 else quad.at[z]
        target[...] = pair[n] + pair[4 + n]
    for step in range(3):
        copy = share(quad.at[z], quad.at[z], 3 + step, partners[3 + step])
        copy.start()
        tail.append(copy)
    for copy in tail[3:]:
        copy.wait_recv()
    total_ref[...] = (quad[0] + quad[1]) + (quad[2] + quad[3])
    for copy in tail:
        copy.wait_send()
    for j in range(count):
        pltpu.make_async_copy(arrive[j][0], arrive[j][0], send_sem.at[j, 0]).wait()
        pltpu.make_async_copy(arrive[j][1], arrive[j][1], send_sem.at[j, 1]).wait()
        pltpu.make_async_copy(arrive[j][2], arrive[j][2], send_sem.at[j, 2]).wait()
        for step in range(3):
            slot = arrive[j][3].at[step]
            pltpu.make_async_copy(slot, slot, send_sem.at[j, 3 + step]).wait()


def scatter_sums(arrays, parts, loss, collective_id):
    sources, chunks, slots, scratch_a, scratch_b = [], [], [], [], []
    for index, (array, cuts) in enumerate(zip(arrays, parts)):
        devices, rows, columns = array.shape
        sources.append(array.reshape(GRID_DIMS + (rows, columns)))
        cut = column_cuts(columns, cuts)
        widest = max(width for low, width in cut)
        base = len(scratch_b)
        scratch_b += [pltpu.VMEM((16, rows, widest), jnp.float32)] * min(2, cuts)
        for number, (low, width) in enumerate(cut):
            chunks.append((index, low, width))
            slots.append((base + number % 2, width))
            scratch_a += [pltpu.VMEM((n, rows, width), jnp.float32) for n in (16, 8, 4, 3)]
    count = len(chunks)
    sent = sum(array.size for array in arrays) * 4
    vmem = pl.BlockSpec(memory_space=pltpu.VMEM)
    return pl.pallas_call(
        functools.partial(scatter_kernel, tuple(chunks), tuple(slots), len(arrays)),
        in_specs=[pl.BlockSpec(memory_space=pl.ANY)] * len(arrays) + [vmem],
        out_specs=[vmem] * (len(arrays) + 1),
        out_shape=[jax.ShapeDtypeStruct(a.shape[1:], jnp.float32) for a in arrays]
        + [jax.ShapeDtypeStruct((2, 8, LANES), jnp.float32)],
        scratch_shapes=scratch_a + scratch_b
        + [
            pltpu.VMEM((7, 2, 8, LANES), jnp.float32),
            pltpu.VMEM((4, 2, 8, LANES), jnp.float32),
            pltpu.SemaphoreType.DMA((count, 6)),
            pltpu.SemaphoreType.DMA((count, 6)),
            pltpu.SemaphoreType.DMA((count,)),
            pltpu.SemaphoreType.DMA((6,)),
            pltpu.SemaphoreType.DMA((6,)),
        ],
        compiler_params=pltpu.CompilerParams(
            collective_id=collective_id, has_side_effects=True, vmem_limit_bytes=63 << 20
        ),
        cost_estimate=pl.CostEstimate(flops=sent // 2, bytes_accessed=3 * sent, transcendentals=0),
        name="scatter_sums",
    )(*sources, loss)


def gather_kernel(chunks, arrays, *refs):
    shards, wholes = refs[:arrays], refs[arrays : 2 * arrays]
    send_sem, recv_sem, own_sem = refs[2 * arrays :]
    x, core, z, y, partners = place_of()
    first, second = xy_of(core, x, y)

    def remote(source, target, j, phase, partner):
        return pltpu.make_async_remote_copy(
            source, target, send_sem.at[j, phase], recv_sem.at[j, phase], device_id=partner, device_id_type=MESH_IDS
        )

    def line(j, b1, b2):
        array, low, width = chunks[j]
        at_x, at_y = xy_of(core, b1, b2)
        return wholes[array].at[at_x, core, :, at_y, :, pl.ds(low, width)]

    def mine(j):
        array, low, width = chunks[j]
        return shards[array].at[:, pl.ds(low, width)], wholes[array].at[x, core, z, y, :, pl.ds(low, width)]

    def along_z(j):
        source, target = mine(j)
        copies = [remote(source, target, j, step, partners[3 + step]) for step in range(3)]
        return copies

    def along_second(j):
        return [remote(line(j, first, second), line(j, first, second), j, 3, partners[2])]

    def along_first(j):
        return [remote(line(j, first, b2), line(j, first, b2), j, 4 + b2, partners[1]) for b2 in range(2)]

    def across(j):
        return [
            remote(line(j, b1, b2), line(j, b1, b2), j, 6 + b1 * 2 + b2, partners[0])
            for b1 in range(2)
            for b2 in range(2)
        ]

    greet(partners)
    count = len(chunks)
    stages = (along_z, along_second, along_first, across)
    flights = [[None] * count for stage in stages]
    for j in range(count):
        source, target = mine(j)
        pltpu.make_async_copy(source, target, own_sem.at[j]).start()
    for t in range(count + len(stages) - 1):
        for s, stage in enumerate(stages):
            j = t - s
            if 0 <= j < count:
                if s == 1:
                    source, target = mine(j)
                    pltpu.make_async_copy(source, target, own_sem.at[j]).wait()
                if s > 0:
                    for copy in flights[s - 1][j]:
                        copy.wait_recv()
                flights[s][j] = stage(j)
                for copy in flights[s][j]:
                    copy.start()
    for j in range(count):
        for copy in flights[-1][j]:
            copy.wait_recv()
    for j in range(count):
        for flight in flights:
            for copy in flight[j]:
                copy.wait_send()


def gather_whole(shards, parts, collective_id):
    chunks = []
    for index, (shard, cuts) in enumerate(zip(shards, parts)):
        chunks += [(index, low, width) for low, width in column_cuts(shard.shape[1], cuts)]
    count = len(chunks)
    wholes = pl.pallas_call(
        functools.partial(gather_kernel, tuple(chunks), len(shards)),
        in_specs=[pl.BlockSpec(memory_space=pltpu.VMEM)] * len(shards),
        out_specs=[pl.BlockSpec(memory_space=pl.ANY)] * len(shards),
        out_shape=[jax.ShapeDtypeStruct(GRID_DIMS + s.shape, s.dtype) for s in shards],
        scratch_shapes=[
            pltpu.SemaphoreType.DMA((count, 10)),
            pltpu.SemaphoreType.DMA((count, 10)),
            pltpu.SemaphoreType.DMA((count,)),
        ],
        compiler_params=pltpu.CompilerParams(
            collective_id=collective_id, has_side_effects=True, vmem_limit_bytes=16 << 20
        ),
        name="gather_whole",
    )(*shards)
    return [w.reshape((math.prod(GRID_DIMS),) + s.shape) for w, s in zip(wholes, shards)]


def vector_tile(vectors):
    joined = jnp.concatenate(vectors, axis=-1)
    lead, length = joined.shape[:-1], joined.shape[-1]
    columns = LANES * (-(-length // (8 * LANES)))
    joined = jnp.pad(joined, [(0, 0)] * len(lead) + [(0, 8 * columns - length)])
    return joined.reshape(lead + (8, columns))


def cut_tile(tile, lengths):
    return pieces(tile.reshape(tile.shape[:-2] + (-1,)), lengths)


def starts_of(widths):
    return [sum(widths[:index]) for index in range(len(widths))]


def wide(array):
    return array.astype(jnp.float32)


def narrow(array):
    return array.astype(jnp.bfloat16)


def per_device(pixels, resolution, kept, step_count, *state):
    masters, firsts, seconds = state[:6], state[6:12], state[12:]
    devices = lax.axis_size("dp") * lax.axis_size("fsdp")
    kernels = (lax.axis_size("dp"), lax.axis_size("fsdp")) == (4, 8)
    count = pixels.shape[0]
    patches_all = count * devices
    denom = (0.75 + 0.1 * 0.25) * patches_all
    groups = count // (SIDE_BIG * SIDE_BIG)
    shards = [narrow(master) for master in masters]
    lengths = [master.shape[0] for master in masters[4:]]
    in_starts, out_starts = starts_of(ENCODER_IN), starts_of(DECODER_IN)

    if kernels:
        tile = vector_tile(shards[4:])
        listed = [(0, 0, tile.shape[1], 1)]
        listed += [(1, low, width, cut) for low, width, cut in zip(in_starts, ENCODER_IN, (1, 2, 1, 2, 1))]
        listed += [(2, 0, D, 2)]
        listed += [(3, low, width, 1) for low, width in zip(out_starts[:2], DECODER_IN[:2])]
        whole = run_alone(Gather([tile] + shards[:3], listed), 1, "gather_first")
        vectors = [v.reshape(-1) for v in cut_tile(whole[0].reshape((devices,) + tile.shape), lengths)]
        early = [wide(w.reshape(-1, w.shape[-1])) for w in whole[1:]]
        gather = Gather(shards[2:4], [(0, out_starts[2], DFF, 2), (0, out_starts[3], PIX, 1), (1, 0, DD, 2)])
    else:
        whole = [lax.all_gather(shard, AXES, axis=0, tiled=True) for shard in shards]
        vectors = whole[4:]
        late = [wide(part) for part in pieces(whole[2], DECODER_IN)]
        early = [wide(part) for part in pieces(whole[0], ENCODER_IN)] + [wide(whole[1])] + late[:2]
        gather = None
    w_patch, w_qkv, w_out, w_up, w_lift, w_down, w_qkv_decoder, w_out_decoder = early
    vectors = [wide(vector) for vector in vectors]
    gains = pieces(vectors[0], ENCODER_GAINS + DECODER_GAINS)
    biases = pieces(vectors[1], ENCODER_BIASES + DECODER_BIASES)
    enc_gains, dec_gains = gains[:3], gains[3:]
    enc_biases, mask_token, dec_biases = biases[:10], biases[10], biases[11:]

    places, old_of_new, kept_new = layout(resolution, kept, count)
    rows, cols, part, run = places(kept_new)
    enc_marks = segment_marks(part * groups + run, 1)
    enc_positions = sine_table(rows, cols, D)
    rows, cols, part, run = places(jnp.arange(count, dtype=jnp.int32))
    dec_marks = segment_marks(part, groups)
    dec_positions = sine_table(rows, cols, DD)
    units = pixels.reshape(-1, SIDE_SMALL * SIDE_SMALL, PIX)
    pixel_rows = wide(units[old_of_new].reshape(count, PIX))
    centered = pixel_rows - jnp.mean(pixel_rows, axis=1, keepdims=True)
    target = centered * lax.rsqrt(jnp.mean(centered * centered, axis=1, keepdims=True) + 1e-06)
    chosen = jnp.any(jnp.arange(count, dtype=jnp.int32)[:, None] == kept_new[None, :], axis=1)
    weight = jnp.where(chosen, 0.1, 1.0)
    kept_pixels = pixels[kept]

    def open_encoder(gains, biases, spare):
        return encoder_open(gains, biases, spare, wide(kept_pixels), enc_positions, w_patch, w_qkv)

    def close_encoder(mixed, stream, gains, biases, spares):
        return encoder_close(mixed, stream, gains, biases, spares, (w_out, w_up, w_down, w_lift))

    def open_decoder(lifted, mask_token, gains, biases, weight_in):
        return decoder_open(lifted, mask_token, gains, biases, kept_new, dec_positions, groups, weight_in)

    def close_decoder(mixed, stream, gains, biases, weights):
        return decoder_close(mixed, stream, gains, biases, weights, target, weight, denom)

    def spare(width):
        return jnp.zeros((kept.shape[0], width), jnp.bfloat16)

    (trio, stream), pull_open, normed = jax.vjp(open_encoder, enc_gains, enc_biases, spare(D), has_aux=True)
    enc_trio = [narrow(t) for t in trio]
    enc_mixed, enc_lse, unused = attend_forward(*enc_trio, enc_marks, HEADS)
    spares = [spare(width) for width in (D, FF, D, DD)]
    lifted, pull_close, saved = jax.vjp(
        close_encoder, wide(enc_mixed), stream, enc_gains, enc_biases, spares, has_aux=True
    )
    (trio, stream), pull_dec_open = jax.vjp(open_decoder, lifted, mask_token, dec_gains, dec_biases, w_qkv_decoder)
    dec_trio = [narrow(t) for t in trio]
    dec_mixed, dec_lse, late_weights = attend_forward(*dec_trio, dec_marks, DHEADS, gather, 2)
    if kernels:
        late = [None, None] + [wide(w.reshape(-1, w.shape[-1])) for w in late_weights]
        w_down_decoder = late[4]
    else:
        w_down_decoder = wide(whole[3])
    dec_weights = (w_out_decoder, late[2], w_down_decoder, late[3])
    loss_local, pull_dec_close = jax.vjp(close_decoder, wide(dec_mixed), stream, dec_gains, dec_biases, dec_weights)

    d_mixed, d_stream, d_gains_a, d_biases_a, d_weights = pull_dec_close(jnp.ones((), jnp.float32))

    def terms_of(array, cuts):
        width = array.shape[1]
        return Terms(array.shape[0] // devices, width, cuts, array=array)

    late_terms = [terms_of(array, cuts) for array, cuts in zip(d_weights, (1, 4, 4, 2))]
    scatter = Scatter(late_terms) if kernels else None
    dec_back, late_sums = attend_backward(
        *dec_trio, narrow(d_mixed), dec_lse, dec_marks, DHEADS, scatter, 3
    )
    d_lifted, d_mask, d_gains_b, d_biases_b, d_qkv = pull_dec_open((tuple(wide(t) for t in dec_back), d_stream))
    d_mixed, d_stream, e_gains_a, e_biases_a, d_spares = pull_close(d_lifted)
    enc_back, unused = attend_backward(*enc_trio, narrow(d_mixed), enc_lse, enc_marks, HEADS)
    e_gains_b, e_biases_b, d_patch = pull_open((tuple(wide(t) for t in enc_back), d_stream))

    def total(a, b):
        return [x + y for x, y in zip(a, b)]

    gain_terms = jnp.concatenate(total(e_gains_a, e_gains_b) + total(d_gains_a, d_gains_b))
    bias_terms = jnp.concatenate(total(e_biases_a, e_biases_b) + [d_mask] + total(d_biases_a, d_biases_b))
    normed_two, active, last = (narrow(value) for value in saved)
    joined_back = jnp.concatenate([t[0] for t in enc_back], axis=0)

    def product(left, right, dims, cuts):
        left_axis, right_axis = dims[0][0][0], dims[0][1][0]
        return Terms(left.shape[1 - left_axis] // devices, right.shape[1 - right_axis], cuts, None, left, right, dims)

    terms = [
        product(last, d_spares[3], CONTRACT_ROWS, 1),
        product(active, d_spares[2], CONTRACT_ROWS, 3),
        product(normed_two, d_spares[1], CONTRACT_ROWS, 4),
        product(enc_mixed[0], d_spares[0], CONTRACT_PLAIN, 1),
        terms_of(d_qkv, 2),
        product(narrow(normed).T, joined_back, CONTRACT_LANES, 3),
        product(kept_pixels, d_patch, CONTRACT_ROWS, 2),
    ]
    if kernels:
        tile = vector_tile([vector.reshape(devices, -1) for vector in (gain_terms, bias_terms)])
        tile_terms = Terms(tile.shape[1], tile.shape[2], 1, array=tile)
        spot = lax.broadcasted_iota(jnp.int32, (8, LANES), 0) + lax.broadcasted_iota(jnp.int32, (8, LANES), 1)
        plan = Scatter(terms[:5] + [tile_terms] + terms[5:], jnp.where(spot == 0, loss_local, 0.0))
        sums = list(run_alone(plan, 4, "scatter_last", late_sums))
        totals = sums.pop()
        vector_sums = cut_tile(sums.pop(5), lengths)
        total_squares, loss_total = jnp.sum(totals[0]), jnp.sum(totals[1])
    else:

        def scattered(array):
            return lax.psum_scatter(array, AXES, scatter_dimension=0, tiled=True)

        sums = [
            scattered(t.array if t.array is not None else tile_dot(t.left, t.right, t.dims)) for t in terms
        ]
        late_sums = [scattered(array) for array in d_weights]
        vector_sums = [scattered(vector) for vector in (gain_terms, bias_terms)]
        squares = sum(jnp.sum(g * g) for g in list(sums) + list(late_sums) + list(vector_sums))
        total_squares, loss_total = lax.psum(squares, AXES), lax.psum(loss_local, AXES)
    g_lift, g_down, g_up, g_out, g_qkv_decoder, g_qkv, g_patch = sums
    g_out_decoder, g_up_decoder, g_down_decoder, g_head = late_sums
    grads = [
        jnp.concatenate([g_patch, g_qkv, g_out, g_up, g_lift], axis=1),
        g_down,
        jnp.concatenate([g_qkv_decoder, g_out_decoder, g_up_decoder, g_head], axis=1),
        g_down_decoder,
    ] + list(vector_sums)
    grad_norm = jnp.sqrt(total_squares)
    factor = jnp.minimum(1.0, 0.5 / math.sqrt(patches_all) / (grad_norm + 1e-06))
    times = step_count[0].astype(jnp.float32)
    results = [
        adamw(
            masters[index],
            grads[index] * factor,
            firsts[index],
            seconds[index],
            DECAY if index < 4 else 0.0,
            times,
        )
        for index in range(6)
    ]
    return (loss_total, grad_norm) + tuple(result[part] for part in range(3) for result in results)


def solution(mesh):
    in_specs = (
        P(("dp", "fsdp"), None),
        P(("dp", "fsdp")),
        P(("dp", "fsdp")),
        P(),
        P(("dp", "fsdp"), None),
        P(("dp", "fsdp"), None),
        P(("dp", "fsdp"), None),
        P(("dp", "fsdp"), None),
        P(("dp", "fsdp")),
        P(("dp", "fsdp")),
        P(("dp", "fsdp"), None),
        P(("dp", "fsdp"), None),
        P(("dp", "fsdp"), None),
        P(("dp", "fsdp"), None),
        P(("dp", "fsdp")),
        P(("dp", "fsdp")),
        P(("dp", "fsdp"), None),
        P(("dp", "fsdp"), None),
        P(("dp", "fsdp"), None),
        P(("dp", "fsdp"), None),
        P(("dp", "fsdp")),
        P(("dp", "fsdp")),
    )
    out_specs = (
        P(),
        P(),
        P(("dp", "fsdp"), None),
        P(("dp", "fsdp"), None),
        P(("dp", "fsdp"), None),
        P(("dp", "fsdp"), None),
        P(("dp", "fsdp")),
        P(("dp", "fsdp")),
        P(("dp", "fsdp"), None),
        P(("dp", "fsdp"), None),
        P(("dp", "fsdp"), None),
        P(("dp", "fsdp"), None),
        P(("dp", "fsdp")),
        P(("dp", "fsdp")),
        P(("dp", "fsdp"), None),
        P(("dp", "fsdp"), None),
        P(("dp", "fsdp"), None),
        P(("dp", "fsdp"), None),
        P(("dp", "fsdp")),
        P(("dp", "fsdp")),
    )
    return jax.shard_map(
        per_device, mesh=mesh, in_specs=in_specs, out_specs=out_specs, check_vma=False
    )
```

```python
import functools
import math

import jax
import jax.numpy as jnp
from jax import lax
from jax.experimental import pallas as pl
from jax.experimental.pallas import tpu as pltpu
from jax.sharding import PartitionSpec as P

D = 768
HEADS = 12
FF = 3072
DD = 512
DHEADS = 16
DFF = 2048
PIX = 768
SIDE_BIG = 28
SIDE_SMALL = 14


BETA_ONE = 0.9
BETA_TWO = 0.95
EPSILON = 1e-08
RATE = 0.05
DECAY = 0.05


def round_plain(value):
    return lax.optimization_barrier(value.astype(jnp.bfloat16)).astype(jnp.float32)


def value_fwd(value):
    return (round_plain(value), None)


def value_bwd(unused, grad):
    return (grad,)


def identity_plain(value):
    return value


def grad_fwd(value):
    return (value, None)


def grad_bwd(unused, grad):
    return (round_plain(grad),)


def make_rounders():
    value_rule = jax.custom_vjp(round_plain)
    value_rule.defvjp(value_fwd, value_bwd)
    grad_rule = jax.custom_vjp(identity_plain)
    grad_rule.defvjp(grad_fwd, grad_bwd)
    return (value_rule, grad_rule)


def value_round(value):
    return make_rounders()[0](value)


def grad_round(value):
    return make_rounders()[1](value)


def matmul(left, right):
    return jnp.dot(left, right, preferred_element_type=jnp.float32)


def both(value):
    return value_round(grad_round(value))


def pieces(vector, widths):
    result = []
    start = 0
    for width in widths:
        result.append(vector[..., start : start + width])
        start += width
    return result


def layout(resolution, kept, count):
    big, small = SIDE_BIG * SIDE_BIG, SIDE_SMALL * SIDE_SMALL
    ratio = big // small
    units = count // small
    is_big = (resolution == 1).astype(jnp.int32)
    is_small = (resolution == 0).astype(jnp.int32)
    bigs = jnp.sum(is_big)
    lengths = ratio * is_big + is_small
    slots = jnp.arange(resolution.shape[0], dtype=jnp.int32)
    before = slots[:, None] > slots[None, :]

    def earlier(values):
        return jnp.sum(jnp.where(before, values[None, :], 0), axis=1)

    old_start = earlier(lengths)
    new_start = jnp.where(resolution == 1, ratio * earlier(is_big), ratio * bigs + earlier(is_small))
    unit = jnp.arange(units, dtype=jnp.int32)[:, None]
    inside = (unit >= old_start[None, :]) & (unit < (old_start + lengths)[None, :])
    new_of_old = jnp.sum(jnp.where(inside, unit + (new_start - old_start)[None, :], 0), axis=1)
    old_of_new = jnp.sum(jnp.where(unit == new_of_old[None, :], jnp.arange(units, dtype=jnp.int32)[None, :], 0), axis=1)
    kept_unit = kept // small
    matches = kept_unit[:, None] == jnp.arange(units, dtype=jnp.int32)[None, :]
    kept_new = jnp.sum(jnp.where(matches, new_of_old[None, :], 0), axis=1) * small + kept % small

    def places(position):
        whole = position < bigs * big
        place = jnp.where(whole, position % big, position % small)
        side = jnp.where(whole, SIDE_BIG, SIDE_SMALL)
        row = place // side
        part = (position % big) // small
        return (row, place - row * side, jnp.where(whole, 0, part), position // big)

    return places, old_of_new, kept_new


def sine_table(row_pos, col_pos, width):
    quarter = width // 4
    reach = 8 * (-(-SIDE_BIG // 8))
    omega = 1.0 / 10000.0 ** (jnp.arange(quarter, dtype=jnp.float32) / quarter)
    angles = jnp.arange(reach, dtype=jnp.float32)[:, None] * omega[None, :]
    half = jnp.concatenate([jnp.sin(angles), jnp.cos(angles)], axis=1)
    none = jnp.zeros_like(half)
    table = jnp.concatenate(
        [jnp.concatenate([half, none], axis=1), jnp.concatenate([none, half], axis=1)], axis=0
    )
    spot = jnp.arange(2 * reach, dtype=jnp.int32)[None, :]
    hot = (spot == row_pos[:, None]) | (spot == col_pos[:, None] + reach)
    return jnp.dot(hot.astype(jnp.float32), table, precision=lax.Precision.HIGHEST)


def layer_norm(stream, gain, shift):
    centered = stream - jnp.mean(stream, axis=1, keepdims=True)
    spread = jnp.mean(centered * centered, axis=1, keepdims=True)
    return centered * lax.rsqrt(spread + 1e-06) * gain + shift


LOG2E = 1.4426950408889634
SEGMENTS = 16
FAR = -1e30
CONTRACT_ROWS = (((0,), (0,)), ((), ()))
CONTRACT_PLAIN = (((1,), (0,)), ((), ()))
CONTRACT_LANES = (((1,), (1,)), ((), ()))


def tile_dot(left, right, dims):
    return lax.dot_general(left, right, dims, preferred_element_type=jnp.float32)


LANES = 128
AXES = ("dp", "fsdp")
GRID_DIMS = (2, 2, 4, 2)
DEVICE_BLOCKS = 32
MESH_IDS = pl.DeviceIdType.MESH
SPACING = 2
WHOLE_VMEM = pl.BlockSpec(memory_space=pltpu.VMEM)
LEFT_ALONE = pl.BlockSpec(memory_space=pl.ANY)


def place_of():
    dp, fsdp = lax.axis_index("dp"), lax.axis_index("fsdp")
    x, core = dp // 2, dp % 2
    z, y = fsdp // 2, fsdp % 2
    flip_x = ((1 - x) * 2 + core, fsdp)
    flip_y = (dp, z * 2 + 1 - y)

    def choose(zero, one):
        return tuple(a * (1 - core) + b * core for a, b in zip(zero, one))

    partners = [(x * 2 + 1 - core, fsdp), choose(flip_x, flip_y), choose(flip_y, flip_x)]
    partners += [(dp, lax.rem(z + step, 4) * 2 + y) for step in (1, 2, 3)]
    return x, core, z, y, partners


def greet(partners):
    barrier = pltpu.get_barrier_semaphore()
    for partner in partners:
        pl.semaphore_signal(barrier, inc=1, device_id=partner, device_id_type=MESH_IDS)
    pl.semaphore_wait(barrier, len(partners))


def column_cuts(columns, parts):
    tiles = columns // LANES
    cuts = [LANES * (tiles * part // parts) for part in range(parts + 1)]
    return [(low, high - low) for low, high in zip(cuts[:-1], cuts[1:])]


def xy_of(core, first, second):
    return first * (1 - core) + second * core, second * (1 - core) + first * core


class Terms:
    def __init__(self, rows, columns, cuts, array=None, left=None, right=None, dims=None):
        self.rows, self.columns, self.cuts = rows, columns, cuts
        self.array, self.left, self.right, self.dims = array, left, right, dims

    def inputs(self):
        if self.array is None:
            return [(self.left, WHOLE_VMEM), (self.right, WHOLE_VMEM)]
        return [(self.array.reshape(GRID_DIMS + (self.rows, self.columns)), LEFT_ALONE)]


class Scatter:
    def __init__(self, terms, loss=None):
        self.terms, self.loss = terms, loss
        pairs = [pair for term in terms for pair in term.inputs()]
        if loss is not None:
            pairs.append((loss, WHOLE_VMEM))
        self.arrays = [array for array, spec in pairs]
        self.in_specs = [spec for array, spec in pairs]
        self.out_shape = [jax.ShapeDtypeStruct((t.rows, t.columns), jnp.float32) for t in terms]
        if loss is not None:
            self.out_shape.append(jax.ShapeDtypeStruct((2, 8, LANES), jnp.float32))
        self.out_specs = [WHOLE_VMEM] * len(self.out_shape)
        self.chunks, self.slots, landing, kept = [], [], [], []
        kinds, last = {}, {}
        for term in terms:
            kind = (term.rows, term.array is None)
            widest = max(width for low, width in column_cuts(term.columns, term.cuts))
            kinds[kind] = (max(widest, kinds.get(kind, (0, 0))[0]), term.cuts + kinds.get(kind, (0, 0))[1])
        bases = {}
        for kind, (widest, number) in kinds.items():
            bases[kind] = (len(kept), min(2, number))
            dims = GRID_DIMS if kind[1] else (16,)
            kept += [pltpu.VMEM(dims + (kind[0], widest), jnp.float32)] * min(2, number)
        seen = {}
        for index, term in enumerate(terms):
            kind = (term.rows, term.array is None)
            for low, width in column_cuts(term.columns, term.cuts):
                base, number = bases[kind]
                slot = base + seen.get(kind, 0) % number
                seen[kind] = seen.get(kind, 0) + 1
                self.chunks.append((index, low, width, last.get(slot)))
                last[slot] = len(self.chunks) - 1
                self.slots.append((slot, width))
                landing += [pltpu.VMEM((n, term.rows, width), jnp.float32) for n in (16, 8, 4, 3)]
        count = len(self.chunks)
        self.kept = len(kept)
        self.scratch = landing + kept
        if loss is not None:
            self.scratch += [pltpu.VMEM((7, 2, 8, LANES), jnp.float32), pltpu.VMEM((4, 2, 8, LANES), jnp.float32)]
            self.scratch += [pltpu.SemaphoreType.DMA((6,)), pltpu.SemaphoreType.DMA((6,))]
        self.scratch += [
            pltpu.SemaphoreType.DMA((count, 6)),
            pltpu.SemaphoreType.DMA((count, 6)),
            pltpu.SemaphoreType.DMA((count,)),
        ]

    def steps(self, ins, outs, scratch):
        chunks, terms, count = self.chunks, self.terms, len(self.chunks)
        sources, at = [], 0
        for term in terms:
            number = 2 if term.array is None else 1
            sources.append(ins[at : at + number])
            at += number
        arrive = [scratch[4 * j : 4 * j + 4] for j in range(count)]
        kept = scratch[4 * count : 4 * count + self.kept]
        send_sem, recv_sem, own_sem = scratch[-3:]
        x, core, z, y, partners = place_of()
        first, second = xy_of(core, x, y)

        def remote(source, target, j, phase, partner):
            return pltpu.make_async_remote_copy(
                source, target, send_sem.at[j, phase], recv_sem.at[j, phase], device_id=partner, device_id_type=MESH_IDS
            )

        def slot_of(j):
            slot, width = self.slots[j]
            lead = 1 if terms[chunks[j][0]].array is not None else 4
            return kept[slot].at[(slice(None),) * lead + (slice(None), pl.ds(0, width))]

        def view(j, side, b1, b2):
            index, low, width, before = chunks[j]
            at_x, at_y = xy_of(side, b1, b2)
            if terms[index].array is None:
                return slot_of(j).at[at_x, side, :, at_y]
            return sources[index][0].at[at_x, side, :, at_y, :, pl.ds(low, width)]

        def sent(j, phase):
            buffer = arrive[j][min(phase, 3)]
            buffer = buffer.at[phase - 3] if phase >= 3 else buffer
            pltpu.make_async_copy(buffer, buffer, send_sem.at[j, phase]).wait()

        def came(j, phase):
            buffer = arrive[j][min(phase, 3)]
            buffer = buffer.at[phase - 3] if phase >= 3 else buffer
            pltpu.make_async_copy(buffer, buffer, recv_sem.at[j, phase]).wait()

        quarters = [(b1, b2, pl.ds((b1 * 2 + b2) * 4, 4)) for b1 in range(2) for b2 in range(2)]

        def begin(j):
            index, low, width, before = chunks[j]
            term = terms[index]
            if term.array is None:
                if before is not None:
                    sent(before, 0)
                left, right = sources[index]
                piece = right[pl.ds(low, width), :] if term.dims == CONTRACT_LANES else right[:, pl.ds(low, width)]
                product = tile_dot(left[...], piece, term.dims)
                slot_of(j)[...] = product.reshape(GRID_DIMS + (term.rows, width))
            for b1, b2, place in quarters:
                remote(view(j, 1 - core, b1, b2), arrive[j][0].at[place], j, 0, partners[0]).start()
                if term.array is not None:
                    pltpu.make_async_copy(view(j, core, b1, b2), slot_of(j).at[place], own_sem.at[j]).start()

        def add_into(target, other, offset, blocks):
            def step(n, carry):
                target[n] = target[n] + other[offset + n]
                return carry

            lax.fori_loop(0, blocks, step, 0)

        def stage_one(j):
            slot = slot_of(j)
            product = terms[chunks[j][0]].array is None
            if not product:
                pltpu.make_async_copy(slot, slot, own_sem.at[j]).wait()
            came(j, 0)
            if product:
                for b1, b2, place in quarters:
                    at_x, at_y = xy_of(core, b1, b2)
                    for at_z in range(4):
                        n = (b1 * 2 + b2) * 4 + at_z
                        arrive[j][0][n] = arrive[j][0][n] + slot[at_x, core, at_z, at_y]
            else:
                add_into(arrive[j][0], slot, 0, 16)
            remote(arrive[j][0].at[pl.ds((1 - first) * 8, 8)], arrive[j][1], j, 1, partners[1]).start()

        def stage_two(j):
            came(j, 1)
            add_into(arrive[j][1], arrive[j][0], first * 8, 8)
            remote(arrive[j][1].at[pl.ds((1 - second) * 4, 4)], arrive[j][2], j, 2, partners[2]).start()

        def stage_three(j):
            came(j, 2)
            add_into(arrive[j][2], arrive[j][1], second * 4, 4)
            for step in range(3):
                there = lax.rem(z + step + 1, 4)
                remote(arrive[j][2].at[there], arrive[j][3].at[step], j, 3 + step, partners[3 + step]).start()

        def stage_four(j):
            index, low, width, before = chunks[j]
            for step in range(3):
                came(j, 3 + step)
            far = arrive[j][3]
            outs[index][:, low : low + width] = (arrive[j][2][z] + far[0]) + (far[1] + far[2])

        def run(t):
            if t == 0:
                greet(partners)
                begin(0)
            if t + 1 < count:
                begin(t + 1)
            for number, stage in enumerate((stage_one, stage_two, stage_three, stage_four)):
                j = t - SPACING * number
                if 0 <= j < count:
                    stage(j)

        def finish():
            again = {before for index, low, width, before in chunks if before is not None and terms[index].array is None}
            for j in range(count):
                for phase in range(6):
                    if phase > 0 or j not in again:
                        sent(j, phase)

        def totals():
            pair, quad, last_send, last_recv = scratch[-7:-3]
            loss_ref, total_ref, square_ins = ins[at], outs[-1], ins[at + 1 :]

            def share(source, target, n, partner):
                return pltpu.make_async_remote_copy(
                    source, target, last_send.at[n], last_recv.at[n], device_id=partner, device_id_type=MESH_IDS
                )

            tile = jnp.zeros((8, LANES), jnp.float32)
            for ref in list(outs[: len(terms)]) + list(square_ins):
                square = ref[...] * ref[...]
                rows, columns = square.shape
                tile = functools.reduce(
                    jnp.add,
                    [square[r : r + 8, c : c + LANES] for r in range(0, rows, 8) for c in range(0, columns, LANES)],
                    tile,
                )
            pair[0, 0] = tile
            pair[0, 1] = loss_ref[...]
            tail = []
            for n in range(3):
                copy = share(pair.at[n], pair.at[4 + n], n, partners[n])
                copy.start()
                copy.wait_recv()
                tail.append(copy)
                target = pair.at[n + 1] if n < 2 else quad.at[z]
                target[...] = pair[n] + pair[4 + n]
            for step in range(3):
                copy = share(quad.at[z], quad.at[z], 3 + step, partners[3 + step])
                copy.start()
                tail.append(copy)
            for copy in tail[3:]:
                copy.wait_recv()
            total_ref[...] = (quad[0] + quad[1]) + (quad[2] + quad[3])
            for copy in tail:
                copy.wait_send()

        parts = [functools.partial(run, t) for t in range(count + 3 * SPACING)]
        return parts + ([totals] if self.loss is not None else []) + [finish]


class Gather:
    def __init__(self, shards, cut_pieces):
        self.arrays, self.in_specs = list(shards), [WHOLE_VMEM] * len(shards)
        self.chunks, self.out_shape = [], []
        for shard, low, width, cuts in cut_pieces:
            for start, wide in column_cuts(width, cuts):
                self.chunks.append((shard, low + start, len(self.out_shape), start, wide))
            self.out_shape.append(
                jax.ShapeDtypeStruct(GRID_DIMS + (shards[shard].shape[0], width), jnp.bfloat16)
            )
        self.out_specs = [LEFT_ALONE] * len(self.out_shape)
        count = len(self.chunks)
        self.scratch = [pltpu.VMEM(shard.shape, jnp.bfloat16) for shard in shards] + [
            pltpu.SemaphoreType.DMA((count, 10)),
            pltpu.SemaphoreType.DMA((count, 10)),
            pltpu.SemaphoreType.DMA((count,)),
        ]

    def steps(self, ins, outs, scratch):
        chunks, count = self.chunks, len(self.chunks)
        sources, rounded = ins, scratch[:-3]
        send_sem, recv_sem, own_sem = scratch[-3:]
        x, core, z, y, partners = place_of()
        first, second = xy_of(core, x, y)

        def remote(source, target, j, phase, partner):
            return pltpu.make_async_remote_copy(
                source, target, send_sem.at[j, phase], recv_sem.at[j, phase], device_id=partner, device_id_type=MESH_IDS
            )

        def line(j, b1, b2):
            shard, source, out, low, width = chunks[j]
            at_x, at_y = xy_of(core, b1, b2)
            return outs[out].at[at_x, core, :, at_y, :, pl.ds(low, width)]

        def mine(j):
            shard, source, out, low, width = chunks[j]
            return rounded[shard].at[:, pl.ds(source, width)], outs[out].at[x, core, z, y, :, pl.ds(low, width)]

        def own(j):
            source, target = mine(j)
            return pltpu.make_async_copy(source, target, own_sem.at[j])

        def along_z(j):
            source, target = mine(j)
            return [remote(source, target, j, step, partners[3 + step]) for step in range(3)]

        def along_second(j):
            return [remote(line(j, first, second), line(j, first, second), j, 3, partners[2])]

        def along_first(j):
            return [remote(line(j, first, b2), line(j, first, b2), j, 4 + b2, partners[1]) for b2 in range(2)]

        def across(j):
            return [
                remote(line(j, b1, b2), line(j, b1, b2), j, 6 + b1 * 2 + b2, partners[0])
                for b1 in range(2)
                for b2 in range(2)
            ]

        stages = (along_z, along_second, along_first, across)

        def run(t):
            if t == 0:
                for source, target in zip(sources, rounded):
                    target[...] = source[...].astype(jnp.bfloat16)
                greet(partners)
                for j in range(count):
                    own(j).start()
            for s, stage in enumerate(stages):
                j = t - SPACING * s
                if 0 <= j < count:
                    if s == 1:
                        own(j).wait()
                    if s > 0:
                        for copy in stages[s - 1](j):
                            copy.wait_recv()
                    for copy in stage(j):
                        copy.start()

        def finish():
            for j in range(count):
                for copy in across(j):
                    copy.wait_recv()
            for j in range(count):
                for stage in stages:
                    for copy in stage(j):
                        copy.wait_send()

        return [functools.partial(run, t) for t in range(count + SPACING * (len(stages) - 1))] + [finish]


def run_alone(plan, collective_id, name, more=()):
    def kernel(*refs):
        inputs = len(plan.arrays) + len(more)
        outputs = len(plan.out_shape)
        for step in plan.steps(refs[:inputs], refs[inputs : inputs + outputs], refs[inputs + outputs :]):
            step()

    sent = sum(array.size * array.dtype.itemsize for array in plan.arrays)
    return pl.pallas_call(
        kernel,
        in_specs=plan.in_specs + [WHOLE_VMEM] * len(more),
        out_specs=plan.out_specs,
        out_shape=plan.out_shape,
        scratch_shapes=plan.scratch,
        compiler_params=pltpu.CompilerParams(
            collective_id=collective_id, has_side_effects=True, vmem_limit_bytes=63 << 20
        ),
        cost_estimate=pl.CostEstimate(flops=sent, bytes_accessed=2 * sent, transcendentals=0),
        name=name,
    )(*plan.arrays, *more)


def hosted_refs(refs, inputs, outputs, plan):
    extra_in = len(plan.arrays) if plan else 0
    extra_out = len(plan.out_shape) if plan else 0
    cuts = [inputs, extra_in, outputs, extra_out]
    result, at = [], 0
    for cut in cuts:
        result.append(refs[at : at + cut])
        at += cut
    own_in, plan_in, own_out, plan_out = result
    steps = plan.steps(plan_in, plan_out, refs[at:]) if plan else []
    return own_in, own_out, steps


def host_steps(steps, heads, head, work):
    blocks = pl.num_programs(1)
    now = (pl.program_id(0) * blocks + pl.program_id(1)) * heads + head
    places = {}
    total = 2 * 16
    for number, step in enumerate(steps[:-1]):
        places.setdefault(number * total // (len(steps) - 1), []).append(step)
    for place, group in places.items():

        @pl.when(now == place)
        def start(group=group):
            for step in group:
                step()

    work()
    if steps:
        pl.when(now == total - 1)(steps[-1])


def attend_fwd_kernel(heads, size, plan, *refs):
    (qkv_ref, away_ref, own_ref), (o_ref, lse_ref), steps = hosted_refs(refs, 3, 2, plan)
    factor = LOG2E / math.sqrt(size)

    def one_head(head, carry):
        def work():
            rows = pl.ds(pl.multiple_of(head * size, size), size)
            queries = jnp.concatenate([qkv_ref[0, 0, rows, :], away_ref[0]], axis=0)
            keys = jnp.concatenate([qkv_ref[0, 1, rows, :], own_ref[0]], axis=0)
            scores = tile_dot(keys, queries, CONTRACT_ROWS)
            top = jnp.max(scores, axis=0, keepdims=True)
            shifted = jnp.exp2((scores - top) * factor)
            total = jnp.sum(shifted, axis=0, keepdims=True)
            weights = (shifted * (1.0 / total)).astype(jnp.bfloat16)
            o_ref[0, rows, :] = tile_dot(qkv_ref[0, 2, rows, :], weights, CONTRACT_PLAIN).astype(o_ref.dtype)
            lse_ref[0, pl.ds(head, 1), :] = top * factor + jnp.log2(total)

        host_steps(steps, heads, head, work)
        return carry

    lax.fori_loop(0, heads, one_head, 0)


def attend_bwd_kernel(heads, size, plan, *refs):
    ins, (back_ref,), steps = hosted_refs(refs, 5, 1, plan)
    qkv_ref, do_ref, lse_ref, away_ref, own_ref = ins
    scale = 1.0 / math.sqrt(size)
    factor = LOG2E * scale

    def one_head(head, carry):
        def work():
            rows = pl.ds(pl.multiple_of(head * size, size), size)
            q_rows, k_rows, do_rows = qkv_ref[0, 0, rows, :], qkv_ref[0, 1, rows, :], do_ref[0, rows, :]
            queries = jnp.concatenate([q_rows, away_ref[0]], axis=0)
            keys = jnp.concatenate([k_rows, own_ref[0]], axis=0)
            scores = tile_dot(keys, queries, CONTRACT_ROWS)
            weights = jnp.exp2(scores * factor - lse_ref[0, pl.ds(head, 1), :])
            spread = tile_dot(qkv_ref[0, 2, rows, :], do_rows, CONTRACT_ROWS)
            product = weights * spread
            inner = jnp.sum(product, axis=0, keepdims=True)
            dscores = (product - weights * inner).astype(jnp.bfloat16)
            rounded = weights.astype(jnp.bfloat16)
            back_ref[0, 2, rows, :] = tile_dot(do_rows, rounded, CONTRACT_LANES).astype(back_ref.dtype)
            back_ref[0, 1, rows, :] = (tile_dot(q_rows, dscores, CONTRACT_LANES) * scale).astype(back_ref.dtype)
            back_ref[0, 0, rows, :] = (tile_dot(k_rows, dscores, CONTRACT_PLAIN) * scale).astype(back_ref.dtype)

        host_steps(steps, heads, head, work)
        return carry

    lax.fori_loop(0, heads, one_head, 0)


def attend_call(kernel, name, trio, grads, lse, marks, heads, plan, collective_id):
    groups, three, width, count = trio.shape
    size = width // heads
    step = 8 if heads % 8 == 0 else heads
    triple = pl.BlockSpec((1, three, step * size, count), lambda g, i: (g, 0, i, 0))
    wide = pl.BlockSpec((1, step * size, count), lambda g, i: (g, i, 0))
    stats = pl.BlockSpec((1, step, count), lambda g, i: (g, i, 0))
    mark = pl.BlockSpec((1, SEGMENTS, count), lambda g, i: (g, 0, 0))
    forward = grads is None
    ins, in_specs = [trio], [triple]
    if forward:
        out_specs = [wide, stats]
        out_shape = [
            jax.ShapeDtypeStruct((groups, width, count), jnp.bfloat16),
            jax.ShapeDtypeStruct((groups, heads, count), jnp.float32),
        ]
    else:
        ins += [grads, lse]
        in_specs += [wide, stats]
        out_specs, out_shape = [triple], [jax.ShapeDtypeStruct(trio.shape, jnp.bfloat16)]
    ins += list(marks)
    in_specs += [mark, mark]
    extra = {}
    if plan is not None:
        ins += plan.arrays
        in_specs += plan.in_specs
        out_specs += plan.out_specs
        out_shape += plan.out_shape
        extra = dict(collective_id=collective_id, has_side_effects=True)
    products = 2 if forward else 5
    return pl.pallas_call(
        functools.partial(kernel, step, size, plan),
        grid=(groups, heads // step),
        in_specs=in_specs,
        out_specs=out_specs,
        out_shape=out_shape,
        scratch_shapes=plan.scratch if plan is not None else [],
        compiler_params=pltpu.CompilerParams(vmem_limit_bytes=62 << 20, **extra),
        cost_estimate=pl.CostEstimate(
            flops=2 * products * groups * width * count * count,
            bytes_accessed=8 * groups * width * count,
            transcendentals=groups * heads * count * count,
        ),
        name=name,
    )(*ins)


def attend_forward(trio, marks, heads, plan=None, collective_id=None):
    outs = attend_call(attend_fwd_kernel, "attend_forward", trio, None, None, marks, heads, plan, collective_id)
    return outs[0], outs[1], outs[2:]


def attend_backward(trio, grads, lse, marks, heads, plan=None, collective_id=None):
    outs = attend_call(attend_bwd_kernel, "attend_backward", trio, grads, lse, marks, heads, plan, collective_id)
    return outs[0], outs[1:]


def gelu(value):
    return 0.5 * value * (1.0 + lax.erf(value * math.sqrt(0.5)))


def segment_marks(segment, groups):
    segment = segment.reshape(groups, 1, -1)
    hot = segment == jnp.arange(SEGMENTS, dtype=jnp.int32)[None, :, None]
    return (jnp.where(hot, 0.0, 1.0).astype(jnp.bfloat16), jnp.where(hot, FAR, 0.0).astype(jnp.bfloat16))


def tap_plain(value, spare):
    return value


def tap_fwd(value, spare):
    return (value, None)


def tap_bwd(unused, grad):
    return (grad, grad.astype(jnp.bfloat16))


def tap(value, spare):
    rule = jax.custom_vjp(tap_plain)
    rule.defvjp(tap_fwd, tap_bwd)
    return rule(value, spare)


ENCODER_GAINS = (D, D, D)
ENCODER_BIASES = (D, D, D, D, D, D, FF, D, D, DD, DD)
DECODER_GAINS = (DD, DD, DD)
DECODER_BIASES = (DD, DD, DD, DD, DD, DFF, DD, DD, PIX)
ENCODER_IN = (D, 3 * D, D, FF, DD)
DECODER_IN = (3 * DD, DD, DFF, PIX)


def heads_in(stream, gain, shift, weight, bias_query, bias_value, groups):
    width = stream.shape[1]
    normed = value_round(layer_norm(stream, gain, shift))
    joined = jnp.einsum(
        "gtd,df->gft", normed.reshape(groups, -1, width), weight, preferred_element_type=jnp.float32
    )
    added = jnp.concatenate([bias_query, jnp.zeros_like(bias_query), bias_value])
    trio = both(joined + added[None, :, None])
    return trio.reshape(groups, 3, width, -1), normed


def encoder_open(gains, biases, spare, pixel_rows, positions, w_patch, w_qkv):
    gain_one = gains[0]
    bias_patch, shift_one, bias_query, bias_value = biases[:4]
    stream = grad_round(tap(matmul(pixel_rows, w_patch), spare) + bias_patch) + positions
    trio, normed = heads_in(stream, gain_one, shift_one, w_qkv, bias_query, bias_value, 1)
    return (trio, stream), normed


def encoder_close(mixed, stream, gains, biases, spares, weights):
    unused, gain_two, gain_final = gains
    bias_out, shift_two, bias_up, bias_down, shift_final, bias_lift = biases[4:10]
    w_out, w_up, w_down, w_lift = weights
    projected = jnp.einsum("gft,fd->gtd", mixed, w_out, preferred_element_type=jnp.float32)
    stream = stream + grad_round(tap(projected[0], spares[0]) + bias_out)
    normed = value_round(layer_norm(stream, gain_two, shift_two))
    hidden = grad_round(tap(matmul(normed, w_up), spares[1]) + bias_up)
    active = value_round(gelu(hidden))
    stream = stream + grad_round(tap(matmul(active, w_down), spares[2]) + bias_down)
    last = value_round(layer_norm(stream, gain_final, shift_final))
    lifted = grad_round(tap(matmul(last, w_lift), spares[3]) + bias_lift)
    return lifted, (normed, active, last)


def decoder_open(lifted, mask_token, gains, biases, kept_new, positions, groups, w_qkv):
    full = jnp.broadcast_to(mask_token[None, :], positions.shape).at[kept_new].set(lifted, unique_indices=True)
    stream = full + positions
    trio, normed = heads_in(stream, gains[0], biases[0], w_qkv, biases[1], biases[2], groups)
    return trio, stream


def decoder_close(mixed, stream, gains, biases, weights, target, weight, denom):
    unused, gain_two, gain_final = gains
    bias_out, shift_two, bias_up, bias_down, shift_final, bias_head = biases[3:]
    w_out, w_up, w_down, w_head = weights
    projected = jnp.einsum("gft,fd->gtd", mixed, w_out, preferred_element_type=jnp.float32)
    stream = stream + grad_round(projected.reshape(stream.shape) + bias_out)
    normed = value_round(layer_norm(stream, gain_two, shift_two))
    hidden = grad_round(matmul(normed, w_up) + bias_up)
    stream = stream + grad_round(matmul(value_round(gelu(hidden)), w_down) + bias_down)
    last = value_round(layer_norm(stream, gain_final, shift_final))
    predicted = grad_round(matmul(last, w_head) + bias_head)
    error = jnp.mean((predicted - target) ** 2, axis=1)
    return jnp.sum(error * weight) / denom


def adamw(weight, grad, first, second, decay, times):
    first_new = BETA_ONE * first + (1.0 - BETA_ONE) * grad
    second_new = BETA_TWO * second + (1.0 - BETA_TWO) * grad * grad
    first_hat = first_new / (1.0 - BETA_ONE**times)
    second_hat = second_new / (1.0 - BETA_TWO**times)
    weight_new = weight - RATE * (first_hat / (jnp.sqrt(second_hat) + EPSILON) + decay * weight)
    return (weight_new, first_new, second_new)


LANES = 128
AXES = ("dp", "fsdp")
GRID_DIMS = (2, 2, 4, 2)
MESH_IDS = pl.DeviceIdType.MESH
SPACING = 2


def place_of():
    dp, fsdp = lax.axis_index("dp"), lax.axis_index("fsdp")
    x, core = dp // 2, dp % 2
    z, y = fsdp // 2, fsdp % 2
    flip_x = ((1 - x) * 2 + core, fsdp)
    flip_y = (dp, z * 2 + 1 - y)

    def choose(zero, one):
        return tuple(a * (1 - core) + b * core for a, b in zip(zero, one))

    partners = [(x * 2 + 1 - core, fsdp), choose(flip_x, flip_y), choose(flip_y, flip_x)]
    partners += [(dp, lax.rem(z + step, 4) * 2 + y) for step in (1, 2, 3)]
    return x, core, z, y, partners


def greet(partners):
    barrier = pltpu.get_barrier_semaphore()
    for partner in partners:
        pl.semaphore_signal(barrier, inc=1, device_id=partner, device_id_type=MESH_IDS)
    pl.semaphore_wait(barrier, len(partners))


def column_cuts(columns, parts):
    tiles = columns // LANES
    cuts = [LANES * (tiles * part // parts) for part in range(parts + 1)]
    return [(low, high - low) for low, high in zip(cuts[:-1], cuts[1:])]


def xy_of(core, first, second):
    return first * (1 - core) + second * core, second * (1 - core) + first * core


def scatter_kernel(chunks, slots, arrays, *refs):
    sources, loss_ref = refs[:arrays], refs[arrays]
    outs, total_ref = refs[arrays + 1 : 2 * arrays + 1], refs[2 * arrays + 1]
    scratch = refs[2 * arrays + 2 :]
    count = len(chunks)
    arrive = [scratch[4 * j : 4 * j + 4] for j in range(count)]
    kept = scratch[4 * count : -7]
    own = [kept[slot].at[:, :, pl.ds(0, width)] for slot, width in slots]
    pair, quad, send_sem, recv_sem, own_sem, last_send, last_recv = scratch[-7:]
    x, core, z, y, partners = place_of()
    first, second = xy_of(core, x, y)

    def remote(source, target, j, phase, partner):
        return pltpu.make_async_remote_copy(
            source, target, send_sem.at[j, phase], recv_sem.at[j, phase], device_id=partner, device_id_type=MESH_IDS
        )

    def view(j, side, b1, b2):
        array, low, width = chunks[j]
        at_x, at_y = xy_of(side, b1, b2)
        return sources[array].at[at_x, side, :, at_y, :, pl.ds(low, width)]

    def start_swap(j):
        for b1 in range(2):
            for b2 in range(2):
                place = pl.ds((b1 * 2 + b2) * 4, 4)
                remote(view(j, 1 - core, b1, b2), arrive[j][0].at[place], j, 0, partners[0]).start()

    def start_own(j):
        for b1 in range(2):
            for b2 in range(2):
                place = pl.ds((b1 * 2 + b2) * 4, 4)
                pltpu.make_async_copy(view(j, core, b1, b2), own[j].at[place], own_sem.at[j]).start()

    def whole(j, phase):
        buffer = arrive[j][phase]
        return pltpu.make_async_copy(buffer, buffer, recv_sem.at[j, phase])

    def add_into(target, other, offset, blocks):
        def step(n, carry):
            target[n] = target[n] + other[offset + n]
            return carry

        lax.fori_loop(0, blocks, step, 0)

    sends = []

    def stage_one(j):
        pltpu.make_async_copy(own[j], own[j], own_sem.at[j]).wait()
        whole(j, 0).wait()
        add_into(arrive[j][0], own[j], 0, 16)
        remote(arrive[j][0].at[pl.ds((1 - first) * 8, 8)], arrive[j][1], j, 1, partners[1]).start()

    def stage_two(j):
        whole(j, 1).wait()
        add_into(arrive[j][1], arrive[j][0], first * 8, 8)
        remote(arrive[j][1].at[pl.ds((1 - second) * 4, 4)], arrive[j][2], j, 2, partners[2]).start()

    def stage_three(j):
        whole(j, 2).wait()
        add_into(arrive[j][2], arrive[j][1], second * 4, 4)
        for step in range(3):
            there = lax.rem(z + step + 1, 4)
            remote(arrive[j][2].at[there], arrive[j][3].at[step], j, 3 + step, partners[3 + step]).start()

    def stage_four(j):
        array, low, width = chunks[j]
        for step in range(3):
            slot = arrive[j][3].at[step]
            pltpu.make_async_copy(slot, slot, recv_sem.at[j, 3 + step]).wait()
        result = (arrive[j][2][z] + arrive[j][3][0]) + (arrive[j][3][1] + arrive[j][3][2])
        outs[array][:, low : low + width] = result
        square = result * result
        rows = square.shape[0]
        tile = functools.reduce(
            jnp.add,
            [square[r : r + 8, c : c + LANES] for r in range(0, rows, 8) for c in range(0, width, LANES)],
        )
        pair[0, 0] = pair[0, 0] + tile

    greet(partners)
    pair[0, 0] = jnp.zeros((8, LANES), jnp.float32)
    pair[0, 1] = loss_ref[...]
    ahead = 2
    for j in range(min(ahead, count)):
        start_swap(j)
        start_own(j)
    for t in range(count + 3):
        if t < count:
            if t + ahead < count:
                start_swap(t + ahead)
            stage_one(t)
            if t + ahead < count:
                start_own(t + ahead)
        if 0 <= t - 1 < count:
            stage_two(t - 1)
        if 0 <= t - 2 < count:
            stage_three(t - 2)
        if 0 <= t - 3 < count:
            stage_four(t - 3)

    def share(source, target, n, partner):
        return pltpu.make_async_remote_copy(
            source, target, last_send.at[n], last_recv.at[n], device_id=partner, device_id_type=MESH_IDS
        )

    tail = []
    for n in range(3):
        copy = share(pair.at[n], pair.at[4 + n], n, partners[n])
        copy.start()
        copy.wait_recv()
        tail.append(copy)
        target = pair.at[n + 1] if n < 2 else quad.at[z]
        target[...] = pair[n] + pair[4 + n]
    for step in range(3):
        copy = share(quad.at[z], quad.at[z], 3 + step, partners[3 + step])
        copy.start()
        tail.append(copy)
    for copy in tail[3:]:
        copy.wait_recv()
    total_ref[...] = (quad[0] + quad[1]) + (quad[2] + quad[3])
    for copy in tail:
        copy.wait_send()
    for j in range(count):
        pltpu.make_async_copy(arrive[j][0], arrive[j][0], send_sem.at[j, 0]).wait()
        pltpu.make_async_copy(arrive[j][1], arrive[j][1], send_sem.at[j, 1]).wait()
        pltpu.make_async_copy(arrive[j][2], arrive[j][2], send_sem.at[j, 2]).wait()
        for step in range(3):
            slot = arrive[j][3].at[step]
            pltpu.make_async_copy(slot, slot, send_sem.at[j, 3 + step]).wait()


def scatter_sums(arrays, parts, loss, collective_id):
    sources, chunks, slots, scratch_a, scratch_b = [], [], [], [], []
    for index, (array, cuts) in enumerate(zip(arrays, parts)):
        devices, rows, columns = array.shape
        sources.append(array.reshape(GRID_DIMS + (rows, columns)))
        cut = column_cuts(columns, cuts)
        widest = max(width for low, width in cut)
        base = len(scratch_b)
        scratch_b += [pltpu.VMEM((16, rows, widest), jnp.float32)] * min(2, cuts)
        for number, (low, width) in enumerate(cut):
            chunks.append((index, low, width))
            slots.append((base + number % 2, width))
            scratch_a += [pltpu.VMEM((n, rows, width), jnp.float32) for n in (16, 8, 4, 3)]
    count = len(chunks)
    sent = sum(array.size for array in arrays) * 4
    vmem = pl.BlockSpec(memory_space=pltpu.VMEM)
    return pl.pallas_call(
        functools.partial(scatter_kernel, tuple(chunks), tuple(slots), len(arrays)),
        in_specs=[pl.BlockSpec(memory_space=pl.ANY)] * len(arrays) + [vmem],
        out_specs=[vmem] * (len(arrays) + 1),
        out_shape=[jax.ShapeDtypeStruct(a.shape[1:], jnp.float32) for a in arrays]
        + [jax.ShapeDtypeStruct((2, 8, LANES), jnp.float32)],
        scratch_shapes=scratch_a + scratch_b
        + [
            pltpu.VMEM((7, 2, 8, LANES), jnp.float32),
            pltpu.VMEM((4, 2, 8, LANES), jnp.float32),
            pltpu.SemaphoreType.DMA((count, 6)),
            pltpu.SemaphoreType.DMA((count, 6)),
            pltpu.SemaphoreType.DMA((count,)),
            pltpu.SemaphoreType.DMA((6,)),
            pltpu.SemaphoreType.DMA((6,)),
        ],
        compiler_params=pltpu.CompilerParams(
            collective_id=collective_id, has_side_effects=True, vmem_limit_bytes=63 << 20
        ),
        cost_estimate=pl.CostEstimate(flops=sent // 2, bytes_accessed=3 * sent, transcendentals=0),
        name="scatter_sums",
    )(*sources, loss)


def gather_kernel(chunks, arrays, *refs):
    shards, wholes = refs[:arrays], refs[arrays : 2 * arrays]
    send_sem, recv_sem, own_sem = refs[2 * arrays :]
    x, core, z, y, partners = place_of()
    first, second = xy_of(core, x, y)

    def remote(source, target, j, phase, partner):
        return pltpu.make_async_remote_copy(
            source, target, send_sem.at[j, phase], recv_sem.at[j, phase], device_id=partner, device_id_type=MESH_IDS
        )

    def line(j, b1, b2):
        array, low, width = chunks[j]
        at_x, at_y = xy_of(core, b1, b2)
        return wholes[array].at[at_x, core, :, at_y, :, pl.ds(low, width)]

    def mine(j):
        array, low, width = chunks[j]
        return shards[array].at[:, pl.ds(low, width)], wholes[array].at[x, core, z, y, :, pl.ds(low, width)]

    def along_z(j):
        source, target = mine(j)
        copies = [remote(source, target, j, step, partners[3 + step]) for step in range(3)]
        return copies

    def along_second(j):
        return [remote(line(j, first, second), line(j, first, second), j, 3, partners[2])]

    def along_first(j):
        return [remote(line(j, first, b2), line(j, first, b2), j, 4 + b2, partners[1]) for b2 in range(2)]

    def across(j):
        return [
            remote(line(j, b1, b2), line(j, b1, b2), j, 6 + b1 * 2 + b2, partners[0])
            for b1 in range(2)
            for b2 in range(2)
        ]

    greet(partners)
    count = len(chunks)
    stages = (along_z, along_second, along_first, across)
    flights = [[None] * count for stage in stages]
    for j in range(count):
        source, target = mine(j)
        pltpu.make_async_copy(source, target, own_sem.at[j]).start()
    for t in range(count + len(stages) - 1):
        for s, stage in enumerate(stages):
            j = t - s
            if 0 <= j < count:
                if s == 1:
                    source, target = mine(j)
                    pltpu.make_async_copy(source, target, own_sem.at[j]).wait()
                if s > 0:
                    for copy in flights[s - 1][j]:
                        copy.wait_recv()
                flights[s][j] = stage(j)
                for copy in flights[s][j]:
                    copy.start()
    for j in range(count):
        for copy in flights[-1][j]:
            copy.wait_recv()
    for j in range(count):
        for flight in flights:
            for copy in flight[j]:
                copy.wait_send()


def gather_whole(shards, parts, collective_id):
    chunks = []
    for index, (shard, cuts) in enumerate(zip(shards, parts)):
        chunks += [(index, low, width) for low, width in column_cuts(shard.shape[1], cuts)]
    count = len(chunks)
    wholes = pl.pallas_call(
        functools.partial(gather_kernel, tuple(chunks), len(shards)),
        in_specs=[pl.BlockSpec(memory_space=pltpu.VMEM)] * len(shards),
        out_specs=[pl.BlockSpec(memory_space=pl.ANY)] * len(shards),
        out_shape=[jax.ShapeDtypeStruct(GRID_DIMS + s.shape, s.dtype) for s in shards],
        scratch_shapes=[
            pltpu.SemaphoreType.DMA((count, 10)),
            pltpu.SemaphoreType.DMA((count, 10)),
            pltpu.SemaphoreType.DMA((count,)),
        ],
        compiler_params=pltpu.CompilerParams(
            collective_id=collective_id, has_side_effects=True, vmem_limit_bytes=16 << 20
        ),
        name="gather_whole",
    )(*shards)
    return [w.reshape((math.prod(GRID_DIMS),) + s.shape) for w, s in zip(wholes, shards)]


def vector_tile(vectors):
    joined = jnp.concatenate(vectors, axis=-1)
    lead, length = joined.shape[:-1], joined.shape[-1]
    columns = LANES * (-(-length // (8 * LANES)))
    joined = jnp.pad(joined, [(0, 0)] * len(lead) + [(0, 8 * columns - length)])
    return joined.reshape(lead + (8, columns))


def cut_tile(tile, lengths):
    return pieces(tile.reshape(tile.shape[:-2] + (-1,)), lengths)


def starts_of(widths):
    return [sum(widths[:index]) for index in range(len(widths))]


def wide(array):
    return array.astype(jnp.float32)


def narrow(array):
    return array.astype(jnp.bfloat16)


def per_device(pixels, resolution, kept, step_count, *state):
    masters, firsts, seconds = state[:6], state[6:12], state[12:]
    devices = lax.axis_size("dp") * lax.axis_size("fsdp")
    kernels = (lax.axis_size("dp"), lax.axis_size("fsdp")) == (4, 8)
    count = pixels.shape[0]
    patches_all = count * devices
    denom = (0.75 + 0.1 * 0.25) * patches_all
    groups = count // (SIDE_BIG * SIDE_BIG)
    lengths = [master.shape[0] for master in masters[4:]]
    in_starts, out_starts = starts_of(ENCODER_IN), starts_of(DECODER_IN)

    if kernels:
        tile = vector_tile(masters[4:])
        listed = [(0, 0, tile.shape[1], 1)]
        listed += [(1, low, width, cut) for low, width, cut in zip(in_starts, ENCODER_IN, (1, 2, 1, 2, 1))]
        listed += [(2, 0, D, 2)]
        listed += [(3, low, width, 1) for low, width in zip(out_starts[:2], DECODER_IN[:2])]
        whole = run_alone(Gather([tile] + list(masters[:3]), listed), 1, "gather_first")
        vectors = [v.reshape(-1) for v in cut_tile(whole[0].reshape((devices,) + tile.shape), lengths)]
        early = [wide(w.reshape(-1, w.shape[-1])) for w in whole[1:]]
        gather = Gather(masters[2:4], [(0, out_starts[2], DFF, 2), (0, out_starts[3], PIX, 1), (1, 0, DD, 2)])
    else:
        whole = [lax.all_gather(narrow(master), AXES, axis=0, tiled=True) for master in masters]
        vectors = whole[4:]
        late = [wide(part) for part in pieces(whole[2], DECODER_IN)]
        early = [wide(part) for part in pieces(whole[0], ENCODER_IN)] + [wide(whole[1])] + late[:2]
        gather = None
    w_patch, w_qkv, w_out, w_up, w_lift, w_down, w_qkv_decoder, w_out_decoder = early
    vectors = [wide(vector) for vector in vectors]
    gains = pieces(vectors[0], ENCODER_GAINS + DECODER_GAINS)
    biases = pieces(vectors[1], ENCODER_BIASES + DECODER_BIASES)
    enc_gains, dec_gains = gains[:3], gains[3:]
    enc_biases, mask_token, dec_biases = biases[:10], biases[10], biases[11:]

    places, old_of_new, kept_new = layout(resolution, kept, count)
    rows, cols, part, run = places(kept_new)
    enc_marks = segment_marks(part * groups + run, 1)
    enc_positions = sine_table(rows, cols, D)
    rows, cols, part, run = places(jnp.arange(count, dtype=jnp.int32))
    dec_marks = segment_marks(part, groups)
    dec_positions = sine_table(rows, cols, DD)
    units = pixels.reshape(-1, SIDE_SMALL * SIDE_SMALL, PIX)
    pixel_rows = wide(units[old_of_new].reshape(count, PIX))
    centered = pixel_rows - jnp.mean(pixel_rows, axis=1, keepdims=True)
    target = centered * lax.rsqrt(jnp.mean(centered * centered, axis=1, keepdims=True) + 1e-06)
    chosen = jnp.any(jnp.arange(count, dtype=jnp.int32)[:, None] == kept_new[None, :], axis=1)
    weight = jnp.where(chosen, 0.1, 1.0)
    kept_pixels = pixels[kept]

    def open_encoder(gains, biases, spare):
        return encoder_open(gains, biases, spare, wide(kept_pixels), enc_positions, w_patch, w_qkv)

    def close_encoder(mixed, stream, gains, biases, spares):
        return encoder_close(mixed, stream, gains, biases, spares, (w_out, w_up, w_down, w_lift))

    def open_decoder(lifted, mask_token, gains, biases, weight_in):
        return decoder_open(lifted, mask_token, gains, biases, kept_new, dec_positions, groups, weight_in)

    def close_decoder(mixed, stream, gains, biases, weights):
        return decoder_close(mixed, stream, gains, biases, weights, target, weight, denom)

    def spare(width):
        return jnp.zeros((kept.shape[0], width), jnp.bfloat16)

    (trio, stream), pull_open, normed = jax.vjp(open_encoder, enc_gains, enc_biases, spare(D), has_aux=True)
    enc_trio = narrow(trio)
    enc_mixed, enc_lse, unused = attend_forward(enc_trio, enc_marks, HEADS)
    spares = [spare(width) for width in (D, FF, D, DD)]
    lifted, pull_close, saved = jax.vjp(
        close_encoder, wide(enc_mixed), stream, enc_gains, enc_biases, spares, has_aux=True
    )
    (trio, stream), pull_dec_open = jax.vjp(open_decoder, lifted, mask_token, dec_gains, dec_biases, w_qkv_decoder)
    dec_trio = narrow(trio)
    dec_mixed, dec_lse, late_weights = attend_forward(dec_trio, dec_marks, DHEADS, gather, 2)
    if kernels:
        late = [None, None] + [wide(w.reshape(-1, w.shape[-1])) for w in late_weights]
        w_down_decoder = late[4]
    else:
        w_down_decoder = wide(whole[3])
    dec_weights = (w_out_decoder, late[2], w_down_decoder, late[3])
    loss_local, pull_dec_close = jax.vjp(close_decoder, wide(dec_mixed), stream, dec_gains, dec_biases, dec_weights)

    d_mixed, d_stream, d_gains_a, d_biases_a, d_weights = pull_dec_close(jnp.ones((), jnp.float32))

    def terms_of(array, cuts):
        width = array.shape[1]
        return Terms(array.shape[0] // devices, width, cuts, array=array)

    late_terms = [terms_of(array, cuts) for array, cuts in zip(d_weights, (1, 4, 4, 2))]
    scatter = Scatter(late_terms) if kernels else None
    dec_back, late_sums = attend_backward(
        dec_trio, narrow(d_mixed), dec_lse, dec_marks, DHEADS, scatter, 3
    )
    d_lifted, d_mask, d_gains_b, d_biases_b, d_qkv = pull_dec_open((wide(dec_back), d_stream))
    d_mixed, d_stream, e_gains_a, e_biases_a, d_spares = pull_close(d_lifted)
    enc_back, unused = attend_backward(enc_trio, narrow(d_mixed), enc_lse, enc_marks, HEADS)
    e_gains_b, e_biases_b, d_patch = pull_open((wide(enc_back), d_stream))

    def total(a, b):
        return [x + y for x, y in zip(a, b)]

    gain_terms = jnp.concatenate(total(e_gains_a, e_gains_b) + total(d_gains_a, d_gains_b))
    bias_terms = jnp.concatenate(total(e_biases_a, e_biases_b) + [d_mask] + total(d_biases_a, d_biases_b))
    normed_two, active, last = (narrow(value) for value in saved)
    joined_back = enc_back.reshape(-1, kept.shape[0])

    def product(left, right, dims, cuts):
        left_axis, right_axis = dims[0][0][0], dims[0][1][0]
        return Terms(left.shape[1 - left_axis] // devices, right.shape[1 - right_axis], cuts, None, left, right, dims)

    terms = [
        product(last, d_spares[3], CONTRACT_ROWS, 1),
        product(active, d_spares[2], CONTRACT_ROWS, 3),
        product(normed_two, d_spares[1], CONTRACT_ROWS, 4),
        product(enc_mixed[0], d_spares[0], CONTRACT_PLAIN, 1),
        terms_of(d_qkv, 2),
        product(narrow(normed).T, joined_back, CONTRACT_LANES, 3),
        product(kept_pixels, d_patch, CONTRACT_ROWS, 2),
    ]
    if kernels:
        tile = vector_tile([vector.reshape(devices, -1) for vector in (gain_terms, bias_terms)])
        tile_terms = Terms(tile.shape[1], tile.shape[2], 1, array=tile)
        spot = lax.broadcasted_iota(jnp.int32, (8, LANES), 0) + lax.broadcasted_iota(jnp.int32, (8, LANES), 1)
        plan = Scatter(terms[:5] + [tile_terms] + terms[5:], jnp.where(spot == 0, loss_local, 0.0))
        sums = list(run_alone(plan, 4, "scatter_last", late_sums))
        totals = sums.pop()
        vector_sums = cut_tile(sums.pop(5), lengths)
        total_squares, loss_total = jnp.sum(totals[0]), jnp.sum(totals[1])
    else:

        def scattered(array):
            return lax.psum_scatter(array, AXES, scatter_dimension=0, tiled=True)

        sums = [
            scattered(t.array if t.array is not None else tile_dot(t.left, t.right, t.dims)) for t in terms
        ]
        late_sums = [scattered(array) for array in d_weights]
        vector_sums = [scattered(vector) for vector in (gain_terms, bias_terms)]
        squares = sum(jnp.sum(g * g) for g in list(sums) + list(late_sums) + list(vector_sums))
        total_squares, loss_total = lax.psum(squares, AXES), lax.psum(loss_local, AXES)
    g_lift, g_down, g_up, g_out, g_qkv_decoder, g_qkv, g_patch = sums
    g_out_decoder, g_up_decoder, g_down_decoder, g_head = late_sums
    grads = [
        jnp.concatenate([g_patch, g_qkv, g_out, g_up, g_lift], axis=1),
        g_down,
        jnp.concatenate([g_qkv_decoder, g_out_decoder, g_up_decoder, g_head], axis=1),
        g_down_decoder,
    ] + list(vector_sums)
    grad_norm = jnp.sqrt(total_squares)
    factor = jnp.minimum(1.0, 0.5 / math.sqrt(patches_all) / (grad_norm + 1e-06))
    times = step_count[0].astype(jnp.float32)
    results = [
        adamw(
            masters[index],
            grads[index] * factor,
            firsts[index],
            seconds[index],
            DECAY if index < 4 else 0.0,
            times,
        )
        for index in range(6)
    ]
    return (loss_total, grad_norm) + tuple(result[part] for part in range(3) for result in results)


def solution(mesh):
    in_specs = (
        P(("dp", "fsdp"), None),
        P(("dp", "fsdp")),
        P(("dp", "fsdp")),
        P(),
        P(("dp", "fsdp"), None),
        P(("dp", "fsdp"), None),
        P(("dp", "fsdp"), None),
        P(("dp", "fsdp"), None),
        P(("dp", "fsdp")),
        P(("dp", "fsdp")),
        P(("dp", "fsdp"), None),
        P(("dp", "fsdp"), None),
        P(("dp", "fsdp"), None),
        P(("dp", "fsdp"), None),
        P(("dp", "fsdp")),
        P(("dp", "fsdp")),
        P(("dp", "fsdp"), None),
        P(("dp", "fsdp"), None),
        P(("dp", "fsdp"), None),
        P(("dp", "fsdp"), None),
        P(("dp", "fsdp")),
        P(("dp", "fsdp")),
    )
    out_specs = (
        P(),
        P(),
        P(("dp", "fsdp"), None),
        P(("dp", "fsdp"), None),
        P(("dp", "fsdp"), None),
        P(("dp", "fsdp"), None),
        P(("dp", "fsdp")),
        P(("dp", "fsdp")),
        P(("dp", "fsdp"), None),
        P(("dp", "fsdp"), None),
        P(("dp", "fsdp"), None),
        P(("dp", "fsdp"), None),
        P(("dp", "fsdp")),
        P(("dp", "fsdp")),
        P(("dp", "fsdp"), None),
        P(("dp", "fsdp"), None),
        P(("dp", "fsdp"), None),
        P(("dp", "fsdp"), None),
        P(("dp", "fsdp")),
        P(("dp", "fsdp")),
    )
    return jax.shard_map(
        per_device, mesh=mesh, in_specs=in_specs, out_specs=out_specs, check_vma=False
    )
```
